512 devices in a mesh: slab: 512 (over z, x, y, core).
Axes of the slice: x: 4, y: 8, z: 8, core: 2. Of those that a mesh axis runs over, the one named last changes fastest.
Arguments:
- start_vectors: float32 [2, 512, 256, 256], P(None, 'slab'), may hold values from -6 to 6
- levels: int32 [512, 256, 256], P('slab'), may hold values from 0 to 15
- energies: float32 [16], replicated, may hold values from -4 to 4
Outputs:
- cheb_field: float32 [2, 512, 256, 256], P(None, 'slab')
- lanczos_diag: float32 [2, 8], replicated
- lanczos_off: float32 [2, 7], replicated
- moments: float32 [2, 6], replicated
The draws below stay inside these ranges and needn't reach their ends.
All inputs are finite; a program needn't handle non-finite values.
Results may differ from the reference program's by a relative error of at most 0.0001.
Values sent between devices are 32-bit elements; how exact they have to be, the bound alone decides.
No kernel may reach another device: no remote copies, remote signals or barrier semaphores. Data moves between devices by JAX's collectives and lax.ppermute only.
A program may use at most 64 MiB of HBM per device.

```python
import jax
import jax.numpy as jnp
from jax import lax

NY = 256
NX = 256
VECS = 2
LANCZOS = 8
LEVELS = 16
NZ = 512


def place_ends(entries, stream_key, low, largest):
    shape = entries.shape
    index_at = [jax.random.randint(jax.random.fold_in(stream_key, axis), (), 0, shape[axis]) for axis in range(len(shape))]
    entries = entries.at[tuple(index_at)].set(low)
    longest = shape.index(max(shape))
    index_at[longest] = (index_at[longest] + 1) % shape[longest]
    return entries.at[tuple(index_at)].set(largest)


def shard_levels(stream_key, shape, cuts, least, largest):
    loudness = 1.0
    for position, blocks in cuts:
        heights = jax.random.uniform(jax.random.fold_in(jax.random.fold_in(stream_key, 6), position), (blocks,), jnp.float32, least / len(cuts), largest / len(cuts))
        loudness = loudness * jnp.repeat(jnp.exp(heights), shape[position] // blocks).reshape((-1,) + (1,) * (len(shape) - 1 - position))
    return loudness


def normal_values(stream_key, extent, spread, most, shards=(), held_as=jnp.bfloat16):
    array = spread * jax.random.normal(stream_key, extent, jnp.float32)
    if shards:
        array = array * shard_levels(stream_key, extent, shards, -0.22, 0.18)
    return jnp.clip(array, -most, most).astype(held_as)


def setup_inputs(seed: int = 0) -> dict:
    arg_keys = jax.random.split(jax.random.key(seed), 4)
    return {
        "start_vectors": normal_values(arg_keys[0], (VECS, NZ, NY, NX), 1.0, 6.0, ((1, 512),), jnp.float32),
        "levels": place_ends(jax.random.randint(arg_keys[1], (NZ, NY, NX), 0, LEVELS), jax.random.fold_in(arg_keys[1], 1), 0, LEVELS - 1).astype(jnp.int32),
        "energies": jnp.clip(jax.random.uniform(arg_keys[2], (LEVELS,), jnp.float32, -4.0, 4.0), -4.0, 4.0),
    }


def hamiltonian(field, onsite):
    beside = jnp.roll(field, 1, 1) + jnp.roll(field, -1, 1)
    beside = beside + jnp.roll(field, 1, 2) + jnp.roll(field, -1, 2)
    beside = beside + jnp.roll(field, 1, 3) + jnp.roll(field, -1, 3)
    return onsite[None] * field - beside

def inner(first, second):
    return lax.optimization_barrier(jnp.sum(first * second, axis=(1, 2, 3)))

def expand(values):
    return values[:, None, None, None]

def reference(start_vectors, levels, energies):
    onsite = jnp.take(energies, levels, axis=0)
    norm0 = inner(start_vectors, start_vectors)
    vector = start_vectors / expand(jnp.sqrt(norm0))
    previous = jnp.zeros_like(vector)
    beta_prev = jnp.zeros((VECS,), jnp.float32)
    alphas = []
    betas = []
    for step in range(LANCZOS):
        work = hamiltonian(vector, onsite) - expand(beta_prev) * previous
        alpha = inner(vector, work)
        alphas.append(alpha)
        if step < LANCZOS - 1:
            work = work - expand(alpha) * vector
            beta = jnp.sqrt(inner(work, work))
            betas.append(beta)
            previous, vector, beta_prev = (vector, work / expand(beta), beta)
    diag = jnp.stack(alphas, axis=1)
    offd = jnp.stack(betas, axis=1)
    zero_col = jnp.zeros((VECS, 1), jnp.float32)
    left = jnp.concatenate([zero_col, offd], axis=1)
    right = jnp.concatenate([offd, zero_col], axis=1)
    emin = lax.optimization_barrier(jnp.min(diag - left - right, axis=1))
    emax = lax.optimization_barrier(jnp.max(diag + left + right, axis=1))
    center = expand((emax + emin) * 0.5)
    half = expand(0.55 * (emax - emin))

    def scaled(field):
        return (hamiltonian(field, onsite) - center * field) / half
    term0 = start_vectors
    term1 = scaled(term0)
    term2 = 2.0 * scaled(term1) - term0
    term3 = 2.0 * scaled(term2) - term1
    first = inner(term0, term1)
    moments = jnp.stack([first, inner(term0, term2), inner(term0, term3), 2.0 * inner(term2, term2) - norm0, 2.0 * inner(term3, term2) - first, 2.0 * inner(term3, term3) - norm0], axis=1) / norm0[:, None]
    return (term3, diag, offd, moments)
```

```python
import functools

import jax
import jax.numpy as jnp
from jax import lax
from jax.experimental import pallas as pl
from jax.experimental.pallas import tpu as pltpu
from jax.sharding import Mesh
from jax.sharding import PartitionSpec as P

LANCZOS = 8
SLAB = ("slab_0", "slab_1", "slab_2", "slab_3")
ROWS = 32
NUDGE = 1e-3
ROUNDING = 2e-7
TOLERANCE = 2e-5
VMEM = pl.BlockSpec(memory_space=pltpu.VMEM)
SMEM = pl.BlockSpec(memory_space=pltpu.SMEM)
PARAMS = pltpu.CompilerParams(vmem_limit_bytes=24 * 1024 * 1024)


def from_behind(block, axis, distance):
    devices = range(lax.axis_size(axis))
    route = [((i - distance) % len(devices), i) for i in devices]
    return lax.ppermute(block, axis, route)


def one_axis_at_a_time(value, axes):
    for axis in axes:
        value = lax.psum(value, axis)
    return value


def inner(first, second):
    return jnp.sum(first * second, axis=(1, 2, 3))


def expand(values):
    return values[:, None, None, None]


def hamiltonian(field, onsite):
    below = from_behind(field, SLAB, 1)
    above = from_behind(field, SLAB, -1)
    beside = jnp.roll(field, 1, 2) + jnp.roll(field, -1, 2)
    beside = beside + jnp.roll(field, 1, 3) + jnp.roll(field, -1, 3)
    return onsite[None] * field - (beside + below + above)


def stepwise(start_vectors, levels, energies):
    level_ids = lax.broadcasted_iota(jnp.int32, (energies.shape[0], 1, 1, 1), 0)
    onsite = jnp.sum(
        jnp.where(levels[None] == level_ids, energies[:, None, None, None], 0.0), axis=0
    )
    vec_count = start_vectors.shape[0]
    norm0 = one_axis_at_a_time(inner(start_vectors, start_vectors), SLAB)

    def lanczos(state, step):
        vector, previous, beta_prev = state
        work = hamiltonian(vector, onsite) - expand(beta_prev) * previous
        alpha = one_axis_at_a_time(inner(vector, work), SLAB)
        work = work - expand(alpha) * vector
        beta = jnp.sqrt(one_axis_at_a_time(inner(work, work), SLAB))
        return (work / expand(beta), vector, beta), (alpha, beta)

    vector = start_vectors / expand(jnp.sqrt(norm0))
    _, (alphas, betas) = lax.scan(
        lanczos,
        (vector, jnp.zeros_like(vector), jnp.zeros((vec_count,), jnp.float32)),
        None,
        length=LANCZOS,
    )
    diag = alphas.T
    offd = betas[: LANCZOS - 1].T
    zero_col = jnp.zeros((vec_count, 1), jnp.float32)
    left = jnp.concatenate([zero_col, offd], axis=1)
    right = jnp.concatenate([offd, zero_col], axis=1)
    emin = jnp.min(diag - left - right, axis=1)
    emax = jnp.max(diag + left + right, axis=1)
    center = expand((emax + emin) * 0.5)
    half = expand(0.55 * (emax - emin))

    def scaled(field):
        return (hamiltonian(field, onsite) - center * field) / half

    term1 = scaled(start_vectors)
    term2 = 2.0 * scaled(term1) - start_vectors
    term3 = 2.0 * scaled(term2) - term1
    local = jnp.stack(
        [
            inner(start_vectors, term1),
            inner(start_vectors, term2),
            inner(start_vectors, term3),
            inner(term2, term2),
            inner(term3, term2),
            inner(term3, term3),
        ],
        axis=0,
    )
    sums = one_axis_at_a_time(local, SLAB)
    moments = (
        jnp.stack(
            [
                sums[0],
                sums[1],
                sums[2],
                2.0 * sums[3] - norm0,
                2.0 * sums[4] - sums[0],
                2.0 * sums[5] - norm0,
            ],
            axis=1,
        )
        / norm0[:, None]
    )
    return (term3, diag, offd, moments)


def onsite_kernel(energies_ref, base_ref, levels_ref, out_ref):
    shift, inverse = base_ref[0], base_ref[1]

    def rows_of(chunk, carry):
        rows = pl.ds(chunk * ROWS, ROWS)
        level = levels_ref[0, rows]
        value = jnp.zeros(level.shape, jnp.float32)
        for index in range(energies_ref.shape[0]):
            value = jnp.where(
                level == index, (energies_ref[index] - shift) * inverse, value
            )
        out_ref[0, rows] = value
        return carry

    lax.fori_loop(0, 256 // ROWS, rows_of, 0)


def advance(below, current, above, onsite, previous, inverse, chunk):
    rows = pl.ds(chunk * ROWS, ROWS)
    before = pl.ds(pl.multiple_of((chunk * ROWS + 248) % 256, 8), 8)
    after = pl.ds(pl.multiple_of((chunk * ROWS + ROWS) % 256, 8), 8)
    middle = current[rows]
    tall = jnp.concatenate([current[before], middle, current[after]], axis=0)
    beside = pltpu.roll(tall, 1, 0)[8 : 8 + ROWS]
    beside = beside + pltpu.roll(tall, ROWS + 15, 0)[8 : 8 + ROWS]
    beside = beside + (pltpu.roll(middle, 1, 1) + pltpu.roll(middle, 255, 1))
    beside = beside + (below[rows] + above[rows])
    result = onsite[rows] * middle - inverse * beside
    if previous is not None:
        result = result - previous[rows]
    return result, middle


def folded(values):
    total = values[:, :128] + values[:, 128:]
    return jnp.sum(total.reshape(ROWS // 8, 8, 128), axis=0)


def round_kernel(first, last, base_ref, *refs):
    refs = list(refs)
    low, own, high = refs[:3]
    refs = refs[3:]
    if first:
        sites = refs.pop(0)
        planes_on = [low.at[2], sites.at[0], sites.at[1], high.at[2]]
        before = [None] * 4
    else:
        onsite, prior = refs[:2]
        refs = refs[2:]
        planes_on = [onsite.at[j] for j in range(4)]
        before = [prior.at[j] for j in range(4)]
    if first:
        one, two, kept, sums = refs
    elif last:
        sums, one = refs
        two = None
    else:
        one, two, sums = refs
    inverse = base_ref[1]
    planes = [low.at[0], low.at[1], own.at[0], own.at[1], high.at[0], high.at[1]]
    zero = jnp.zeros((8, 128), jnp.float32)

    def first_half(chunk, carry):
        square0, cross0, square1 = carry
        rows = pl.ds(chunk * ROWS, ROWS)
        for j in range(4):
            new, middle = advance(
                planes[j], planes[j + 1], planes[j + 2], planes_on[j], before[j],
                inverse, chunk,
            )
            one[j, rows] = new
            if first:
                kept[j, rows] = planes_on[j][rows]
            if j in (1, 2):
                if first:
                    square0 = square0 + folded(middle * middle)
                cross0 = cross0 + folded(new * middle)
                square1 = square1 + folded(new * new)
        return square0, cross0, square1

    square0, cross0, square1 = lax.fori_loop(
        0, 256 // ROWS, first_half, (zero, zero, zero)
    )

    def second_half(chunk, carry):
        cross1, square2 = carry
        rows = pl.ds(chunk * ROWS, ROWS)
        for j in range(2):
            new, middle = advance(
                one.at[j], one.at[j + 1], one.at[j + 2], planes_on[j + 1],
                planes[j + 2], inverse, chunk,
            )
            if two is not None:
                two[j, rows] = new
                square2 = square2 + folded(new * new)
            cross1 = cross1 + folded(new * middle)
        return cross1, square2

    cross1, square2 = lax.fori_loop(0, 256 // ROWS, second_half, (zero, zero))
    for index, value in enumerate((square0, cross0, square1, cross1, square2)):
        sums[index] = value


def shape(*dims):
    return jax.ShapeDtypeStruct(dims, jnp.float32)


ROUND_COST = pl.CostEstimate(flops=4_000_000, bytes_accessed=5_000_000, transcendentals=0)


def first_round(base, low, own, high, sites):
    return pl.pallas_call(
        functools.partial(round_kernel, True, False),
        out_shape=(
            shape(4, 256, 256), shape(2, 256, 256), shape(4, 256, 256), shape(5, 8, 128),
        ),
        in_specs=[SMEM] + [VMEM] * 4,
        out_specs=(VMEM,) * 4,
        compiler_params=PARAMS,
        cost_estimate=ROUND_COST,
        name="first_round",
    )(base, low, own, high, sites)


def middle_round(base, low, own, high, onsite, prior):
    return pl.pallas_call(
        functools.partial(round_kernel, False, False),
        out_shape=(shape(4, 256, 256), shape(2, 256, 256), shape(5, 8, 128)),
        in_specs=[SMEM] + [VMEM] * 5,
        out_specs=(VMEM,) * 3,
        compiler_params=PARAMS,
        cost_estimate=ROUND_COST,
        name="middle_round",
    )(base, low, own, high, onsite, prior)


def last_round(base, low, own, high, onsite, prior):
    return pl.pallas_call(
        functools.partial(round_kernel, False, True),
        out_shape=shape(5, 8, 128),
        in_specs=[SMEM] + [VMEM] * 5,
        out_specs=VMEM,
        scratch_shapes=[pltpu.VMEM((4, 256, 256), jnp.float32)],
        compiler_params=PARAMS,
        cost_estimate=ROUND_COST,
        name="last_round",
    )(base, low, own, high, onsite, prior)


def pack_kernel(a_ref, b_ref, c_ref, d_ref, out_ref):
    lane = lax.broadcasted_iota(jnp.int32, (8, 128), 1)
    row = jnp.zeros((8, 128), jnp.float32)
    for index, ref in enumerate((a_ref, b_ref, c_ref, d_ref)):
        places = [None, 8 + 2 * index, 2 * index + 1, 9 + 2 * index, 2 * index + 2]
        if index == 0:
            places[0] = 0
        if index == 3:
            places[4] = None
        for entry, place in enumerate(places):
            if place is None:
                continue
            total = jnp.sum(jnp.sum(ref[entry], axis=0, keepdims=True), axis=1, keepdims=True)
            row = jnp.where(lane == place, total, row)
    out_ref[...] = row[:1]


def pack(sums):
    return pl.pallas_call(
        pack_kernel,
        out_shape=shape(1, 128),
        in_specs=[VMEM] * 4,
        out_specs=VMEM,
        compiler_params=PARAMS,
        name="pack_sums",
    )(*sums)


def finish_kernel(
    base_ref, side_ref, rows_ref, p0, p1, p2, p3,
    field_ref, diag_ref, offd_ref, moments_ref, good_ref,
):
    shift, scale = base_ref[0], base_ref[2]
    lane = lax.broadcasted_iota(jnp.int32, (2, 128), 1)
    rows = rows_ref[...]
    sub = lax.broadcasted_iota(jnp.int32, rows.shape, 0)
    even = jnp.sum(jnp.where(sub % 2 == 0, rows, 0.0), axis=0, keepdims=True)
    odd = jnp.sum(jnp.where(sub % 2 == 1, rows, 0.0), axis=0, keepdims=True)
    total = jnp.concatenate([even, odd], axis=0)

    def column(index):
        return jnp.broadcast_to(total[:, index : index + 1], (2, 128))

    plain = [column(index) for index in range(8)]
    largest = [jnp.maximum(plain[k], plain[min(k + 1, 7)]) for k in range(8)]
    square = [
        plain[k] + jnp.where(lane == k + 1, NUDGE * plain[k], 0.0) for k in range(8)
    ]
    cross = [
        column(8 + k) + jnp.where(lane == k + 9, NUDGE * largest[k], 0.0) for k in range(8)
    ]
    moment = []
    for k in range(8):
        moment.append(square[k] - square[k - 1] if k else square[k])
        moment.append(cross[k] - cross[k - 1] if k else cross[k])
    norm0 = moment[0]
    sigma = [value / norm0 for value in moment]
    normal = list(sigma)
    zero = jnp.zeros_like(norm0)
    older = [zero] * len(sigma)
    alphas, betas = [], []
    weight = zero
    for k in range(LANCZOS):
        size = len(sigma)
        pushed = [
            (sigma[l + 1] + sigma[l - 1]) if l else sigma[1] for l in range(size - 1)
        ]
        ratio = (pushed[k] - weight * older[k]) / sigma[k]
        alphas.append(ratio)
        if k < LANCZOS - 1:
            fresh = [
                pushed[l] - ratio * sigma[l] - weight * older[l] for l in range(size - 1)
            ]
            weight = fresh[k + 1] / sigma[k]
            betas.append(jnp.sqrt(weight))
            older, sigma = sigma, fresh
    alphas = [scale * value + shift for value in alphas]
    betas = [scale * value for value in betas]

    def spread(values):
        error, norm = zero, zero
        for value in values:
            exact = jnp.broadcast_to(value[:, :1], value.shape)
            error = error + jnp.square(
                jnp.broadcast_to(
                    jnp.sum(jnp.abs(value - exact), axis=1, keepdims=True), value.shape
                )
            )
            norm = norm + jnp.square(exact)
        error = jnp.sum(error, axis=0, keepdims=True)
        norm = jnp.sum(norm, axis=0, keepdims=True)
        allowed = TOLERANCE * NUDGE / ROUNDING
        return jnp.where(error <= allowed * allowed * norm, 1, 0)

    fits = jnp.minimum(spread(alphas), spread(betas))
    good_ref[0] = jnp.min(fits)

    lows, highs = [], []
    for k in range(LANCZOS):
        left = betas[k - 1] if k else zero
        right = betas[k] if k < LANCZOS - 1 else zero
        lows.append(alphas[k] - left - right)
        highs.append(alphas[k] + left + right)
    emin = functools.reduce(jnp.minimum, lows)
    emax = functools.reduce(jnp.maximum, highs)
    center = (emax + emin) * 0.5
    half = 0.55 * (emax - emin)
    offset = (shift - center) / half
    factor = scale / half

    def apply(coefs):
        out = []
        for l in range(len(coefs) + 1):
            value = zero
            if l < len(coefs):
                value = value + offset * coefs[l]
            if l + 1 < len(coefs):
                value = value + factor * coefs[l + 1]
            if l:
                value = value + factor * coefs[l - 1]
            out.append(value)
        return out

    terms = [[zero + 1.0]]
    terms.append(apply(terms[0]))
    for m in range(2, 7):
        nxt = apply(terms[-1])
        old = terms[-2]
        terms.append(
            [2.0 * v - (old[l] if l < len(old) else zero) for l, v in enumerate(nxt)]
        )
    diag, offd, out = zero, zero, zero
    for k in range(LANCZOS):
        diag = jnp.where(lane == k, jnp.broadcast_to(alphas[k][:, :1], lane.shape), diag)
        if k < LANCZOS - 1:
            offd = jnp.where(lane == k, jnp.broadcast_to(betas[k][:, :1], lane.shape), offd)
    for m in range(1, 7):
        value = functools.reduce(
            jnp.add, [c * normal[l] for l, c in enumerate(terms[m])]
        )
        out = jnp.where(lane == m - 1, jnp.broadcast_to(value[:, :1], lane.shape), out)
    diag_ref[...] = diag[:, :8]
    offd_ref[...] = offd[:, :7]
    moments_ref[...] = out[:, :6]

    upper = side_ref[0] == 1
    weights = []
    for l in range(4):
        value = jnp.broadcast_to(terms[3][l][:, :1], lane.shape)
        pick = jnp.where(upper, value[1:2], value[0:1])
        weights.append(jnp.concatenate([pick, pick], axis=1))
    sources = [
        [p0.at[0], p0.at[1]],
        [p1.at[1], p1.at[2]],
        [p2.at[0], p2.at[1]],
        [p3.at[1], p3.at[2]],
    ]

    def combine(chunk, carry):
        at = pl.ds(chunk * ROWS, ROWS)
        for j in range(2):
            value = weights[0] * sources[0][j][at]
            for l in range(1, 4):
                value = value + weights[l] * sources[l][j][at]
            field_ref[j, at] = value
        return carry

    lax.fori_loop(0, 256 // ROWS, combine, 0)


def finish(base, side, rows, p0, p1, p2, p3):
    return pl.pallas_call(
        finish_kernel,
        out_shape=(
            shape(2, 256, 256), shape(2, 8), shape(2, 7), shape(2, 6),
            jax.ShapeDtypeStruct((1,), jnp.int32),
        ),
        in_specs=[SMEM, SMEM] + [VMEM] * 5,
        out_specs=(VMEM,) * 4 + (SMEM,),
        compiler_params=PARAMS,
        name="finish",
    )(base, side, rows, p0, p1, p2, p3)


def gathered(row, axes, count):
    copies = jnp.broadcast_to(row[None], (count,) + row.shape)
    return lax.all_to_all(copies, axes, 0, 0, tiled=True).reshape(count, 128)


def shards(start_vectors, levels, energies):
    mean = jnp.mean(energies)
    scale = 1.05 * jnp.sqrt(6.0 + jnp.mean(jnp.square(energies - mean)))
    base = jnp.stack([mean, 1.0 / scale, scale])
    side = lax.axis_index("slab_3").astype(jnp.int32).reshape(1)

    sites_here = pl.pallas_call(
        onsite_kernel,
        out_shape=shape(1, 256, 256),
        in_specs=[SMEM, SMEM, VMEM],
        out_specs=VMEM,
        compiler_params=PARAMS,
        name="onsite",
    )(energies, base, levels)
    own = lax.all_to_all(start_vectors, "slab_3", 0, 1, tiled=True)[0]
    sites = lax.all_gather(sites_here, "slab_3", axis=0, tiled=True)
    upward = jnp.concatenate([own, sites[1:2]], axis=0)
    downward = jnp.concatenate([own, sites[0:1]], axis=0)
    low = from_behind(upward, SLAB, 2)
    high = from_behind(downward, SLAB, -2)
    p1, p2, onsite, sums0 = first_round(base, low, own, high, sites)
    low, high = from_behind(p2, SLAB, 2), from_behind(p2, SLAB, -2)
    p3, p4, sums1 = middle_round(base, low, p2, high, onsite, p1)
    low, high = from_behind(p4, SLAB, 2), from_behind(p4, SLAB, -2)
    p5, p6, sums2 = middle_round(base, low, p4, high, onsite, p3)
    low, high = from_behind(p6, SLAB, 2), from_behind(p6, SLAB, -2)
    sums3 = last_round(base, low, p6, high, onsite, p5)
    row = pack((sums0, sums1, sums2, sums3))
    rows = gathered(row, ("slab_0", "slab_1"), 32)
    rows = gathered(jnp.sum(rows, axis=0, keepdims=True), ("slab_2", "slab_3"), 16)
    field, diag, offd, moments, good = finish(base, side, rows, own, p1, p2, p3)

    def accept(field, diag, offd, moments, *_):
        out = lax.all_to_all(field[None], "slab_3", 1, 0, tiled=True)
        return (out, diag, offd, moments)

    def redo(field, diag, offd, moments, *inputs):
        return stepwise(*inputs)

    return lax.cond(
        good[0] == 1, accept, redo,
        field, diag, offd, moments, start_vectors, levels, energies,
    )


def solution(mesh):
    split = Mesh(mesh.devices.reshape(8, 4, 8, 2), SLAB)
    in_specs = (P(None, SLAB, None, None), P(SLAB, None, None), P())
    out_specs = (P(None, SLAB, None, None), P(), P(), P())
    return jax.shard_map(
        shards, mesh=split, in_specs=in_specs, out_specs=out_specs, check_vma=False
    )
```

```python
import functools

import jax
import jax.numpy as jnp
from jax import lax
from jax.experimental import pallas as pl
from jax.experimental.pallas import tpu as pltpu
from jax.sharding import Mesh
from jax.sharding import PartitionSpec as P

LANCZOS = 8
SLAB = ("slab_0", "slab_1", "slab_2", "slab_3")
ROWS = 32
NUDGE = 1e-3
ROUNDING = 2e-7
TOLERANCE = 1e-4
VMEM = pl.BlockSpec(memory_space=pltpu.VMEM)
SMEM = pl.BlockSpec(memory_space=pltpu.SMEM)
PARAMS = pltpu.CompilerParams(vmem_limit_bytes=24 * 1024 * 1024)


def from_behind(block, axis, distance):
    devices = range(lax.axis_size(axis))
    route = [((i - distance) % len(devices), i) for i in devices]
    return lax.ppermute(block, axis, route)


def one_axis_at_a_time(value, axes):
    for axis in axes:
        value = lax.psum(value, axis)
    return value


def inner(first, second):
    return jnp.sum(first * second, axis=(1, 2, 3))


def expand(values):
    return values[:, None, None, None]


def hamiltonian(field, onsite):
    below = from_behind(field, SLAB, 1)
    above = from_behind(field, SLAB, -1)
    beside = jnp.roll(field, 1, 2) + jnp.roll(field, -1, 2)
    beside = beside + jnp.roll(field, 1, 3) + jnp.roll(field, -1, 3)
    return onsite[None] * field - (beside + below + above)


def stepwise(start_vectors, levels, energies):
    level_ids = lax.broadcasted_iota(jnp.int32, (energies.shape[0], 1, 1, 1), 0)
    onsite = jnp.sum(
        jnp.where(levels[None] == level_ids, energies[:, None, None, None], 0.0), axis=0
    )
    vec_count = start_vectors.shape[0]
    norm0 = one_axis_at_a_time(inner(start_vectors, start_vectors), SLAB)

    def lanczos(state, step):
        vector, previous, beta_prev = state
        work = hamiltonian(vector, onsite) - expand(beta_prev) * previous
        alpha = one_axis_at_a_time(inner(vector, work), SLAB)
        work = work - expand(alpha) * vector
        beta = jnp.sqrt(one_axis_at_a_time(inner(work, work), SLAB))
        return (work / expand(beta), vector, beta), (alpha, beta)

    vector = start_vectors / expand(jnp.sqrt(norm0))
    _, (alphas, betas) = lax.scan(
        lanczos,
        (vector, jnp.zeros_like(vector), jnp.zeros((vec_count,), jnp.float32)),
        None,
        length=LANCZOS,
    )
    diag = alphas.T
    offd = betas[: LANCZOS - 1].T
    zero_col = jnp.zeros((vec_count, 1), jnp.float32)
    left = jnp.concatenate([zero_col, offd], axis=1)
    right = jnp.concatenate([offd, zero_col], axis=1)
    emin = jnp.min(diag - left - right, axis=1)
    emax = jnp.max(diag + left + right, axis=1)
    center = expand((emax + emin) * 0.5)
    half = expand(0.55 * (emax - emin))

    def scaled(field):
        return (hamiltonian(field, onsite) - center * field) / half

    term1 = scaled(start_vectors)
    term2 = 2.0 * scaled(term1) - start_vectors
    term3 = 2.0 * scaled(term2) - term1
    local = jnp.stack(
        [
            inner(start_vectors, term1),
            inner(start_vectors, term2),
            inner(start_vectors, term3),
            inner(term2, term2),
            inner(term3, term2),
            inner(term3, term3),
        ],
        axis=0,
    )
    sums = one_axis_at_a_time(local, SLAB)
    moments = (
        jnp.stack(
            [
                sums[0],
                sums[1],
                sums[2],
                2.0 * sums[3] - norm0,
                2.0 * sums[4] - sums[0],
                2.0 * sums[5] - norm0,
            ],
            axis=1,
        )
        / norm0[:, None]
    )
    return (term3, diag, offd, moments)


def onsite_kernel(energies_ref, base_ref, levels_ref, out_ref):
    shift, inverse = base_ref[0], base_ref[1]

    def rows_of(chunk, carry):
        rows = pl.ds(chunk * ROWS, ROWS)
        level = levels_ref[0, rows]
        value = jnp.zeros(level.shape, jnp.float32)
        for index in range(energies_ref.shape[0]):
            value = jnp.where(
                level == index, (energies_ref[index] - shift) * inverse, value
            )
        out_ref[0, rows] = value
        return carry

    lax.fori_loop(0, 256 // ROWS, rows_of, 0)


def advance(below, current, above, onsite, previous, inverse, chunk):
    rows = pl.ds(chunk * ROWS, ROWS)
    before = pl.ds(pl.multiple_of((chunk * ROWS + 248) % 256, 8), 8)
    after = pl.ds(pl.multiple_of((chunk * ROWS + ROWS) % 256, 8), 8)
    middle = current[rows]
    tall = jnp.concatenate([current[before], middle, current[after]], axis=0)
    beside = pltpu.roll(tall, 1, 0)[8 : 8 + ROWS]
    beside = beside + pltpu.roll(tall, ROWS + 15, 0)[8 : 8 + ROWS]
    beside = beside + (pltpu.roll(middle, 1, 1) + pltpu.roll(middle, 255, 1))
    beside = beside + (below[rows] + above[rows])
    result = onsite[rows] * middle - inverse * beside
    if previous is not None:
        result = result - previous[rows]
    return result, middle


def folded(values):
    total = values[:, :128] + values[:, 128:]
    return jnp.sum(total.reshape(ROWS // 8, 8, 128), axis=0)


def round_kernel(first, last, base_ref, *refs):
    refs = list(refs)
    low, own, high = refs[:3]
    refs = refs[3:]
    if first:
        sites = refs.pop(0)
        planes_on = [low.at[2], sites.at[0], sites.at[1], high.at[2]]
        before = [None] * 4
    else:
        onsite, prior = refs[:2]
        refs = refs[2:]
        planes_on = [onsite.at[j] for j in range(4)]
        before = [prior.at[j] for j in range(4)]
    if first:
        one, two, kept, sums = refs
    elif last:
        sums, one = refs
        two = None
    else:
        one, two, sums = refs
    inverse = base_ref[1]
    planes = [low.at[0], low.at[1], own.at[0], own.at[1], high.at[0], high.at[1]]
    zero = jnp.zeros((8, 128), jnp.float32)

    def first_half(chunk, carry):
        square0, cross0, square1 = carry
        rows = pl.ds(chunk * ROWS, ROWS)
        for j in range(4):
            new, middle = advance(
                planes[j], planes[j + 1], planes[j + 2], planes_on[j], before[j],
                inverse, chunk,
            )
            one[j, rows] = new
            if first:
                kept[j, rows] = planes_on[j][rows]
            if j in (1, 2):
                if first:
                    square0 = square0 + folded(middle * middle)
                cross0 = cross0 + folded(new * middle)
                square1 = square1 + folded(new * new)
        return square0, cross0, square1

    square0, cross0, square1 = lax.fori_loop(
        0, 256 // ROWS, first_half, (zero, zero, zero)
    )

    def second_half(chunk, carry):
        cross1, square2 = carry
        rows = pl.ds(chunk * ROWS, ROWS)
        for j in range(2):
            new, middle = advance(
                one.at[j], one.at[j + 1], one.at[j + 2], planes_on[j + 1],
                planes[j + 2], inverse, chunk,
            )
            if two is not None:
                two[j, rows] = new
                square2 = square2 + folded(new * new)
            cross1 = cross1 + folded(new * middle)
        return cross1, square2

    cross1, square2 = lax.fori_loop(0, 256 // ROWS, second_half, (zero, zero))
    for index, value in enumerate((square0, cross0, square1, cross1, square2)):
        sums[index] = value


def shape(*dims):
    return jax.ShapeDtypeStruct(dims, jnp.float32)


ROUND_COST = pl.CostEstimate(flops=4_000_000, bytes_accessed=5_000_000, transcendentals=0)


def first_round(base, low, own, high, sites):
    return pl.pallas_call(
        functools.partial(round_kernel, True, False),
        out_shape=(
            shape(4, 256, 256), shape(2, 256, 256), shape(4, 256, 256), shape(5, 8, 128),
        ),
        in_specs=[SMEM] + [VMEM] * 4,
        out_specs=(VMEM,) * 4,
        compiler_params=PARAMS,
        cost_estimate=ROUND_COST,
        name="first_round",
    )(base, low, own, high, sites)


def middle_round(base, low, own, high, onsite, prior):
    return pl.pallas_call(
        functools.partial(round_kernel, False, False),
        out_shape=(shape(4, 256, 256), shape(2, 256, 256), shape(5, 8, 128)),
        in_specs=[SMEM] + [VMEM] * 5,
        out_specs=(VMEM,) * 3,
        compiler_params=PARAMS,
        cost_estimate=ROUND_COST,
        name="middle_round",
    )(base, low, own, high, onsite, prior)


def last_round(base, low, own, high, onsite, prior):
    return pl.pallas_call(
        functools.partial(round_kernel, False, True),
        out_shape=shape(5, 8, 128),
        in_specs=[SMEM] + [VMEM] * 5,
        out_specs=VMEM,
        scratch_shapes=[pltpu.VMEM((4, 256, 256), jnp.float32)],
        compiler_params=PARAMS,
        cost_estimate=ROUND_COST,
        name="last_round",
    )(base, low, own, high, onsite, prior)


def pack_kernel(a_ref, b_ref, c_ref, d_ref, out_ref):
    lane = lax.broadcasted_iota(jnp.int32, (8, 128), 1)
    row = jnp.zeros((8, 128), jnp.float32)
    for index, ref in enumerate((a_ref, b_ref, c_ref, d_ref)):
        places = [None, 8 + 2 * index, 2 * index + 1, 9 + 2 * index, 2 * index + 2]
        if index == 0:
            places[0] = 0
        if index == 3:
            places[4] = None
        for entry, place in enumerate(places):
            if place is None:
                continue
            total = jnp.sum(jnp.sum(ref[entry], axis=0, keepdims=True), axis=1, keepdims=True)
            row = jnp.where(lane == place, total, row)
    out_ref[...] = row[:1]


def pack(sums):
    return pl.pallas_call(
        pack_kernel,
        out_shape=shape(1, 128),
        in_specs=[VMEM] * 4,
        out_specs=VMEM,
        compiler_params=PARAMS,
        name="pack_sums",
    )(*sums)


def finish_kernel(
    base_ref, side_ref, rows_ref, p0, p1, p2, p3,
    field_ref, diag_ref, offd_ref, moments_ref, good_ref,
):
    shift, scale = base_ref[0], base_ref[2]
    lane = lax.broadcasted_iota(jnp.int32, (2, 128), 1)
    rows = rows_ref[...]
    sub = lax.broadcasted_iota(jnp.int32, rows.shape, 0)
    even = jnp.sum(jnp.where(sub % 2 == 0, rows, 0.0), axis=0, keepdims=True)
    odd = jnp.sum(jnp.where(sub % 2 == 1, rows, 0.0), axis=0, keepdims=True)
    total = jnp.concatenate([even, odd], axis=0)

    def column(index):
        return jnp.broadcast_to(total[:, index : index + 1], (2, 128))

    plain = [column(index) for index in range(8)]
    largest = [jnp.maximum(plain[k], plain[min(k + 1, 7)]) for k in range(8)]
    square = [
        plain[k] + jnp.where(lane == k + 1, NUDGE * plain[k], 0.0) for k in range(8)
    ]
    cross = [
        column(8 + k) + jnp.where(lane == k + 9, NUDGE * largest[k], 0.0) for k in range(8)
    ]
    moment = []
    for k in range(8):
        moment.append(square[k] - square[k - 1] if k else square[k])
        moment.append(cross[k] - cross[k - 1] if k else cross[k])
    norm0 = moment[0]
    sigma = [value / norm0 for value in moment]
    normal = list(sigma)
    zero = jnp.zeros_like(norm0)
    older = [zero] * len(sigma)
    alphas, betas = [], []
    weight = zero
    for k in range(LANCZOS):
        size = len(sigma)
        pushed = [
            (sigma[l + 1] + sigma[l - 1]) if l else sigma[1] for l in range(size - 1)
        ]
        ratio = (pushed[k] - weight * older[k]) / sigma[k]
        alphas.append(ratio)
        if k < LANCZOS - 1:
            fresh = [
                pushed[l] - ratio * sigma[l] - weight * older[l] for l in range(size - 1)
            ]
            weight = fresh[k + 1] / sigma[k]
            betas.append(jnp.sqrt(weight))
            older, sigma = sigma, fresh
    alphas = [scale * value + shift for value in alphas]
    betas = [scale * value for value in betas]

    def spread(values):
        error, norm = zero, zero
        for value in values:
            exact = jnp.broadcast_to(value[:, :1], value.shape)
            error = error + jnp.square(
                jnp.broadcast_to(
                    jnp.sum(jnp.abs(value - exact), axis=1, keepdims=True), value.shape
                )
            )
            norm = norm + jnp.square(exact)
        error = jnp.sum(error, axis=0, keepdims=True)
        norm = jnp.sum(norm, axis=0, keepdims=True)
        allowed = TOLERANCE * NUDGE / ROUNDING
        return jnp.where(error <= allowed * allowed * norm, 1, 0)

    fits = jnp.minimum(spread(alphas), spread(betas))
    good_ref[0] = jnp.min(fits)

    lows, highs = [], []
    for k in range(LANCZOS):
        left = betas[k - 1] if k else zero
        right = betas[k] if k < LANCZOS - 1 else zero
        lows.append(alphas[k] - left - right)
        highs.append(alphas[k] + left + right)
    emin = functools.reduce(jnp.minimum, lows)
    emax = functools.reduce(jnp.maximum, highs)
    center = (emax + emin) * 0.5
    half = 0.55 * (emax - emin)
    offset = (shift - center) / half
    factor = scale / half

    def apply(coefs):
        out = []
        for l in range(len(coefs) + 1):
            value = zero
            if l < len(coefs):
                value = value + offset * coefs[l]
            if l + 1 < len(coefs):
                value = value + factor * coefs[l + 1]
            if l:
                value = value + factor * coefs[l - 1]
            out.append(value)
        return out

    terms = [[zero + 1.0]]
    terms.append(apply(terms[0]))
    for m in range(2, 7):
        nxt = apply(terms[-1])
        old = terms[-2]
        terms.append(
            [2.0 * v - (old[l] if l < len(old) else zero) for l, v in enumerate(nxt)]
        )
    diag, offd, out = zero, zero, zero
    for k in range(LANCZOS):
        diag = jnp.where(lane == k, jnp.broadcast_to(alphas[k][:, :1], lane.shape), diag)
        if k < LANCZOS - 1:
            offd = jnp.where(lane == k, jnp.broadcast_to(betas[k][:, :1], lane.shape), offd)
    for m in range(1, 7):
        value = functools.reduce(
            jnp.add, [c * normal[l] for l, c in enumerate(terms[m])]
        )
        out = jnp.where(lane == m - 1, jnp.broadcast_to(value[:, :1], lane.shape), out)
    diag_ref[...] = diag[:, :8]
    offd_ref[...] = offd[:, :7]
    moments_ref[...] = out[:, :6]

    upper = side_ref[0] == 1
    weights = []
    for l in range(4):
        value = jnp.broadcast_to(terms[3][l][:, :1], lane.shape)
        pick = jnp.where(upper, value[1:2], value[0:1])
        weights.append(jnp.concatenate([pick, pick], axis=1))
    sources = [
        [p0.at[0], p0.at[1]],
        [p1.at[1], p1.at[2]],
        [p2.at[0], p2.at[1]],
        [p3.at[1], p3.at[2]],
    ]

    def combine(chunk, carry):
        at = pl.ds(chunk * ROWS, ROWS)
        for j in range(2):
            value = weights[0] * sources[0][j][at]
            for l in range(1, 4):
                value = value + weights[l] * sources[l][j][at]
            field_ref[j, at] = value
        return carry

    lax.fori_loop(0, 256 // ROWS, combine, 0)


def finish(base, side, rows, p0, p1, p2, p3):
    return pl.pallas_call(
        finish_kernel,
        out_shape=(
            shape(2, 256, 256), shape(2, 8), shape(2, 7), shape(2, 6),
            jax.ShapeDtypeStruct((1,), jnp.int32),
        ),
        in_specs=[SMEM, SMEM] + [VMEM] * 5,
        out_specs=(VMEM,) * 4 + (SMEM,),
        compiler_params=PARAMS,
        name="finish",
    )(base, side, rows, p0, p1, p2, p3)


def gathered(row, axes, count):
    copies = jnp.broadcast_to(row[None], (count,) + row.shape)
    return lax.all_to_all(copies, axes, 0, 0, tiled=True).reshape(count, 128)


def shards(start_vectors, levels, energies):
    mean = jnp.mean(energies)
    scale = 1.05 * jnp.sqrt(6.0 + jnp.mean(jnp.square(energies - mean)))
    base = jnp.stack([mean, 1.0 / scale, scale])
    side = lax.axis_index("slab_3").astype(jnp.int32).reshape(1)

    sites_here = pl.pallas_call(
        onsite_kernel,
        out_shape=shape(1, 256, 256),
        in_specs=[SMEM, SMEM, VMEM],
        out_specs=VMEM,
        compiler_params=PARAMS,
        name="onsite",
    )(energies, base, levels)
    own = lax.all_to_all(start_vectors, "slab_3", 0, 1, tiled=True)[0]
    sites = lax.all_gather(sites_here, "slab_3", axis=0, tiled=True)
    upward = jnp.concatenate([own, sites[1:2]], axis=0)
    downward = jnp.concatenate([own, sites[0:1]], axis=0)
    low = from_behind(upward, SLAB, 2)
    high = from_behind(downward, SLAB, -2)
    p1, p2, onsite, sums0 = first_round(base, low, own, high, sites)
    low, high = from_behind(p2, SLAB, 2), from_behind(p2, SLAB, -2)
    p3, p4, sums1 = middle_round(base, low, p2, high, onsite, p1)
    low, high = from_behind(p4, SLAB, 2), from_behind(p4, SLAB, -2)
    p5, p6, sums2 = middle_round(base, low, p4, high, onsite, p3)
    low, high = from_behind(p6, SLAB, 2), from_behind(p6, SLAB, -2)
    sums3 = last_round(base, low, p6, high, onsite, p5)
    row = pack((sums0, sums1, sums2, sums3))
    rows = gathered(row, ("slab_0", "slab_1"), 32)
    rows = gathered(jnp.sum(rows, axis=0, keepdims=True), ("slab_2", "slab_3"), 16)
    field, diag, offd, moments, good = finish(base, side, rows, own, p1, p2, p3)

    def accept(field, diag, offd, moments, *_):
        out = lax.all_to_all(field[None], "slab_3", 1, 0, tiled=True)
        return (out, diag, offd, moments)

    def redo(field, diag, offd, moments, *inputs):
        return stepwise(*inputs)

    return lax.cond(
        good[0] == 1, accept, redo,
        field, diag, offd, moments, start_vectors, levels, energies,
    )


def solution(mesh):
    split = Mesh(mesh.devices.reshape(8, 4, 8, 2), SLAB)
    in_specs = (P(None, SLAB, None, None), P(SLAB, None, None), P())
    out_specs = (P(None, SLAB, None, None), P(), P(), P())
    return jax.shard_map(
        shards, mesh=split, in_specs=in_specs, out_specs=out_specs, check_vma=False
    )
```

```python
import functools

import jax
import jax.numpy as jnp
from jax import lax
from jax.experimental import pallas as pl
from jax.experimental.pallas import tpu as pltpu
from jax.sharding import Mesh
from jax.sharding import PartitionSpec as P

LANCZOS = 8
SLAB = ("slab_0", "slab_1", "slab_2", "slab_3")
STAGES = (("slab_1", "slab_2"), ("slab_0", "slab_3"))
ROWS = 32
NUDGE = 1e-3
ROUNDING = 2e-7
TOLERANCE = 1e-4
VMEM = pl.BlockSpec(memory_space=pltpu.VMEM)
SMEM = pl.BlockSpec(memory_space=pltpu.SMEM)
PARAMS = pltpu.CompilerParams(vmem_limit_bytes=24 * 1024 * 1024)


def from_behind(block, axis, distance):
    devices = range(lax.axis_size(axis))
    route = [((i - distance) % len(devices), i) for i in devices]
    return lax.ppermute(block, axis, route)


def one_axis_at_a_time(value, axes):
    for axis in axes:
        value = lax.psum(value, axis)
    return value


def inner(first, second):
    return jnp.sum(first * second, axis=(1, 2, 3))


def expand(values):
    return values[:, None, None, None]


def hamiltonian(field, onsite):
    below = from_behind(field, SLAB, 1)
    above = from_behind(field, SLAB, -1)
    beside = jnp.roll(field, 1, 2) + jnp.roll(field, -1, 2)
    beside = beside + jnp.roll(field, 1, 3) + jnp.roll(field, -1, 3)
    return onsite[None] * field - (beside + below + above)


def stepwise(start_vectors, levels, energies):
    level_ids = lax.broadcasted_iota(jnp.int32, (energies.shape[0], 1, 1, 1), 0)
    onsite = jnp.sum(
        jnp.where(levels[None] == level_ids, energies[:, None, None, None], 0.0), axis=0
    )
    vec_count = start_vectors.shape[0]
    norm0 = one_axis_at_a_time(inner(start_vectors, start_vectors), SLAB)

    def lanczos(state, step):
        vector, previous, beta_prev = state
        work = hamiltonian(vector, onsite) - expand(beta_prev) * previous
        alpha = one_axis_at_a_time(inner(vector, work), SLAB)
        work = work - expand(alpha) * vector
        beta = jnp.sqrt(one_axis_at_a_time(inner(work, work), SLAB))
        return (work / expand(beta), vector, beta), (alpha, beta)

    vector = start_vectors / expand(jnp.sqrt(norm0))
    _, (alphas, betas) = lax.scan(
        lanczos,
        (vector, jnp.zeros_like(vector), jnp.zeros((vec_count,), jnp.float32)),
        None,
        length=LANCZOS,
    )
    diag = alphas.T
    offd = betas[: LANCZOS - 1].T
    zero_col = jnp.zeros((vec_count, 1), jnp.float32)
    left = jnp.concatenate([zero_col, offd], axis=1)
    right = jnp.concatenate([offd, zero_col], axis=1)
    emin = jnp.min(diag - left - right, axis=1)
    emax = jnp.max(diag + left + right, axis=1)
    center = expand((emax + emin) * 0.5)
    half = expand(0.55 * (emax - emin))

    def scaled(field):
        return (hamiltonian(field, onsite) - center * field) / half

    term1 = scaled(start_vectors)
    term2 = 2.0 * scaled(term1) - start_vectors
    term3 = 2.0 * scaled(term2) - term1
    local = jnp.stack(
        [
            inner(start_vectors, term1),
            inner(start_vectors, term2),
            inner(start_vectors, term3),
            inner(term2, term2),
            inner(term3, term2),
            inner(term3, term3),
        ],
        axis=0,
    )
    sums = one_axis_at_a_time(local, SLAB)
    moments = (
        jnp.stack(
            [
                sums[0],
                sums[1],
                sums[2],
                2.0 * sums[3] - norm0,
                2.0 * sums[4] - sums[0],
                2.0 * sums[5] - norm0,
            ],
            axis=1,
        )
        / norm0[:, None]
    )
    return (term3, diag, offd, moments)


def shape(*dims):
    return jax.ShapeDtypeStruct(dims, jnp.float32)


PLANES = shape(2, 256, 256)
CHUNKS = 256 // ROWS
PAIR_COST = pl.CostEstimate(flops=4_000_000, bytes_accessed=4_000_000, transcendentals=0)


def call(kernel, out_shape, in_specs, name, scratch=()):
    return pl.pallas_call(
        kernel,
        out_shape=out_shape,
        in_specs=in_specs,
        out_specs=jax.tree.map(
            lambda leaf: SMEM if leaf.dtype == jnp.int32 else VMEM, out_shape
        ),
        scratch_shapes=scratch,
        compiler_params=PARAMS,
        cost_estimate=PAIR_COST,
        name=name,
    )


def onsite_kernel(energies_ref, levels_ref, out_ref, base_ref):
    count = energies_ref.shape[0]
    row = jnp.zeros((1, 256), jnp.float32)
    values = [row + energies_ref[index] for index in range(count)]
    mean = functools.reduce(jnp.add, values) * (1.0 / count)
    spread = functools.reduce(jnp.add, [jnp.square(v - mean) for v in values])
    scale = 1.05 * jnp.sqrt(6.0 + spread * (1.0 / count))
    inverse = 1.0 / scale
    base_ref[0:1] = mean
    base_ref[1:2] = inverse
    base_ref[2:3] = scale
    base_ref[3:4] = inverse * inverse
    values = [(v - mean) * inverse for v in values]

    def rows_of(chunk, carry):
        rows = pl.ds(chunk * ROWS, ROWS)
        level = levels_ref[0, rows]
        value = jnp.zeros(level.shape, jnp.float32)
        for index in range(count):
            value = jnp.where(level == index, values[index], value)
        out_ref[0, rows] = value
        return carry

    lax.fori_loop(0, CHUNKS, rows_of, 0)


def in_plane(plane, chunk):
    rows = pl.ds(chunk * ROWS, ROWS)
    before = pl.ds(pl.multiple_of((chunk * ROWS + 248) % 256, 8), 8)
    after = pl.ds(pl.multiple_of((chunk * ROWS + ROWS) % 256, 8), 8)
    middle = plane[rows]
    tall = jnp.concatenate([plane[before], middle, plane[after]], axis=0)
    beside = pltpu.roll(tall, 1, 0)[8 : 8 + ROWS]
    beside = beside + pltpu.roll(tall, ROWS + 15, 0)[8 : 8 + ROWS]
    return beside + (pltpu.roll(middle, 1, 1) + pltpu.roll(middle, 255, 1)), middle


def folded(values):
    total = values[:, :128] + values[:, 128:]
    return jnp.sum(total.reshape(ROWS // 8, 8, 128), axis=0)


def chunks(body, count):
    zero = jnp.zeros((8, 128), jnp.float32)
    return lax.fori_loop(0, CHUNKS, body, (zero,) * count)


def before_kernel(first, base_ref, own, sites, *refs):
    if first:
        first_ref, second_ref, sums = refs
    else:
        prior, older, first_ref, second_ref, sums = refs
    inverse = base_ref[1:2]

    def once(chunk, carry):
        rows = pl.ds(chunk * ROWS, ROWS)
        for j in range(2):
            beside, middle = in_plane(own.at[j], chunk)
            value = sites[j, rows] * middle - inverse * (beside + own[1 - j, rows])
            if first:
                carry = (carry[0] + folded(middle * middle),)
            else:
                last = prior[j, rows]
                value = value - last
                carry = (
                    carry[0] + folded(last * older[j, rows]),
                    carry[1] + folded(last * last),
                    carry[2] + folded(middle * last),
                    carry[3] + folded(middle * middle),
                )
            first_ref[j, rows] = value
        return carry

    totals = chunks(once, 1 if first else 4)

    def twice(chunk, carry):
        rows = pl.ds(chunk * ROWS, ROWS)
        for j in range(2):
            beside, middle = in_plane(first_ref.at[j], chunk)
            beside = beside + first_ref[1 - j, rows]
            second_ref[j, rows] = sites[j, rows] * middle - inverse * beside - own[j, rows]
        return carry

    chunks(twice, 0)
    for index, total in enumerate(totals):
        sums[index] = total


def after_kernel(first, last, side_ref, base_ref, even_ref, odd_ref, own, sites, one, two, *refs):
    refs = list(refs)
    if not first:
        edge_sites, edge_prior = refs[:2]
        refs = refs[2:]
    if last:
        parts, row_ref = refs[:4], refs[4]
    else:
        new_one, new_two, new_edge = refs[:3]
        kept = refs[3] if first else None
    inverse, inverse2 = base_ref[1:2], base_ref[3:4]

    def run(low, high):
        def body(chunk, carry):
            rows = pl.ds(chunk * ROWS, ROWS)
            near, far = (low.at[1], high.at[0]), (low.at[0], high.at[1])
            found = [in_plane(plane, chunk) for plane in near]
            for j in range(2):
                beside, middle = found[j]
                if first:
                    site = (low if j == 0 else high)[2, rows]
                    kept[j, rows] = site
                else:
                    site = edge_sites[j, rows]
                mine = own[j, rows]
                edge = site * middle - inverse * (beside + far[j][rows] + mine)
                if not first:
                    edge = edge - edge_prior[j, rows]
                value = one[j, rows] - inverse * middle
                new = two[j, rows] - inverse * (sites[j, rows] * middle + edge)
                new = new + inverse2 * (beside + found[1 - j][1])
                if last:
                    carry = (
                        carry[0] + folded(value * mine),
                        carry[1] + folded(value * value),
                        carry[2] + folded(new * value),
                    )
                else:
                    new_one[j, rows] = value
                    new_two[j, rows] = new
                    new_edge[j, rows] = edge
            return carry

        totals = chunks(body, 3 if last else 0)
        if last:
            pack(parts, totals, row_ref)

    @pl.when(side_ref[1] == 0)
    def _():
        run(odd_ref, even_ref)

    @pl.when(side_ref[1] == 1)
    def _():
        run(even_ref, odd_ref)


def pack(parts, totals, row_ref):
    entries = [(0, parts[0][0])]
    for index in range(3):
        places = (8 + 2 * index, 2 * index + 1, 9 + 2 * index, 2 * index + 2)
        entries += [(place, parts[index + 1][k]) for k, place in enumerate(places)]
    entries += list(zip((14, 7, 15), totals))
    lane = lax.broadcasted_iota(jnp.int32, (1, 128), 1)
    row = jnp.zeros((1, 128), jnp.float32)
    for place, value in entries:
        total = jnp.sum(jnp.sum(value, axis=0, keepdims=True), axis=1, keepdims=True)
        row = jnp.where(lane == place, total, row)
    row_ref[...] = row


def swap_kernel(side_ref, p1, p2, p3, out_ref):
    other = 1 - side_ref[0]

    def body(chunk, carry):
        rows = pl.ds(chunk * ROWS, ROWS)
        for index, ref in enumerate((p1, p2, p3)):
            out_ref[index, rows] = ref[other, rows]
        return carry

    chunks(body, 0)


def finish_kernel(
    side_ref, base_ref, rows_ref, start, p1, p2, p3, swapped,
    field_ref, diag_ref, offd_ref, moments_ref, good_ref,
):
    shift, scale = base_ref[0:1, :128], base_ref[2:3, :128]
    lane = lax.broadcasted_iota(jnp.int32, (2, 128), 1)
    rows = rows_ref[...]
    sub = lax.broadcasted_iota(jnp.int32, rows.shape, 0)
    even = jnp.sum(jnp.where(sub % 2 == 0, rows, 0.0), axis=0, keepdims=True)
    odd = jnp.sum(jnp.where(sub % 2 == 1, rows, 0.0), axis=0, keepdims=True)
    total = jnp.concatenate([even, odd], axis=0)

    def column(index):
        return jnp.broadcast_to(total[:, index : index + 1], (2, 128))

    plain = [column(index) for index in range(8)]
    largest = [jnp.maximum(plain[k], plain[min(k + 1, 7)]) for k in range(8)]
    square = [
        plain[k] + jnp.where(lane == k + 1, NUDGE * plain[k], 0.0) for k in range(8)
    ]
    cross = [
        column(8 + k) + jnp.where(lane == k + 9, NUDGE * largest[k], 0.0) for k in range(8)
    ]
    moment = []
    for k in range(8):
        moment.append(square[k] - square[k - 1] if k else square[k])
        moment.append(cross[k] - cross[k - 1] if k else cross[k])
    norm0 = moment[0]
    sigma = [value / norm0 for value in moment]
    normal = list(sigma)
    zero = jnp.zeros_like(norm0)
    older = [zero] * len(sigma)
    alphas, betas = [], []
    weight = zero
    for k in range(LANCZOS):
        size = len(sigma)
        pushed = [
            (sigma[l + 1] + sigma[l - 1]) if l else sigma[1] for l in range(size - 1)
        ]
        ratio = (pushed[k] - weight * older[k]) / sigma[k]
        alphas.append(ratio)
        if k < LANCZOS - 1:
            fresh = [
                pushed[l] - ratio * sigma[l] - weight * older[l] for l in range(size - 1)
            ]
            weight = fresh[k + 1] / sigma[k]
            betas.append(jnp.sqrt(weight))
            older, sigma = sigma, fresh
    alphas = [scale * value + shift for value in alphas]
    betas = [scale * value for value in betas]

    def spread(values):
        error, norm = zero, zero
        for value in values:
            exact = jnp.broadcast_to(value[:, :1], value.shape)
            error = error + jnp.square(
                jnp.broadcast_to(
                    jnp.sum(jnp.abs(value - exact), axis=1, keepdims=True), value.shape
                )
            )
            norm = norm + jnp.square(exact)
        error = jnp.sum(error, axis=0, keepdims=True)
        norm = jnp.sum(norm, axis=0, keepdims=True)
        allowed = TOLERANCE * NUDGE / ROUNDING
        return jnp.where(error <= allowed * allowed * norm, 1, 0)

    fits = jnp.minimum(spread(alphas), spread(betas))
    good_ref[0] = jnp.min(fits)

    lows, highs = [], []
    for k in range(LANCZOS):
        left = betas[k - 1] if k else zero
        right = betas[k] if k < LANCZOS - 1 else zero
        lows.append(alphas[k] - left - right)
        highs.append(alphas[k] + left + right)
    emin = functools.reduce(jnp.minimum, lows)
    emax = functools.reduce(jnp.maximum, highs)
    center = (emax + emin) * 0.5
    half = 0.55 * (emax - emin)
    offset = (shift - center) / half
    factor = scale / half

    def apply(coefs):
        out = []
        for l in range(len(coefs) + 1):
            value = zero
            if l < len(coefs):
                value = value + offset * coefs[l]
            if l + 1 < len(coefs):
                value = value + factor * coefs[l + 1]
            if l:
                value = value + factor * coefs[l - 1]
            out.append(value)
        return out

    terms = [[zero + 1.0]]
    terms.append(apply(terms[0]))
    for m in range(2, 7):
        nxt = apply(terms[-1])
        old = terms[-2]
        terms.append(
            [2.0 * v - (old[l] if l < len(old) else zero) for l, v in enumerate(nxt)]
        )
    diag, offd, out = zero, zero, zero
    for k in range(LANCZOS):
        diag = jnp.where(lane == k, jnp.broadcast_to(alphas[k][:, :1], lane.shape), diag)
        if k < LANCZOS - 1:
            offd = jnp.where(lane == k, jnp.broadcast_to(betas[k][:, :1], lane.shape), offd)
    for m in range(1, 7):
        value = functools.reduce(
            jnp.add, [c * normal[l] for l, c in enumerate(terms[m])]
        )
        out = jnp.where(lane == m - 1, jnp.broadcast_to(value[:, :1], lane.shape), out)
    diag_ref[...] = diag[:, :8]
    offd_ref[...] = offd[:, :7]
    moments_ref[...] = out[:, :6]

    here = side_ref[0]
    wide = [
        jnp.concatenate([jnp.broadcast_to(terms[3][l][:, :1], lane.shape)] * 2, axis=1)
        for l in range(4)
    ]
    mine = [jnp.where(here == 1, w[1:2], w[0:1]) for w in wide]
    other = [jnp.where(here == 1, w[0:1], w[1:2]) for w in wide]

    def combine(chunk, carry):
        at = pl.ds(chunk * ROWS, ROWS)
        value = mine[0] * start[here, 0, at]
        for l, ref in enumerate((p1, p2, p3)):
            value = value + mine[l + 1] * ref[here, at]
        field_ref[here, 0, at] = value
        value = other[0] * start[1 - here, 0, at]
        for l in range(3):
            value = value + other[l + 1] * swapped[l, at]
        field_ref[1 - here, 0, at] = value
        return carry

    chunks(combine, 0)


def gathered(row, axes, count):
    copies = jnp.broadcast_to(row[None], (count,) + row.shape)
    return lax.all_to_all(copies, axes, 0, 0, tiled=True).reshape(count, 128)


def exchange(block, route):
    return lax.ppermute(block, SLAB, route)


def shards(start_vectors, levels, energies):
    devices = 512
    inside = [(i, i ^ 2) for i in range(devices)]
    across = [(i, (((i + 2) ^ 2) - 2) % devices) for i in range(devices)]
    partner = [(i, i ^ 1) for i in range(devices)]
    core = lax.axis_index("slab_3").astype(jnp.int32)
    parity = lax.axis_index("slab_2").astype(jnp.int32) % 2
    side = jnp.stack([core, parity])

    sites_here, base = call(
        onsite_kernel, (shape(1, 256, 256), shape(8, 256)), [SMEM, VMEM], "onsite"
    )(energies, levels)
    own = lax.all_to_all(start_vectors, "slab_3", 0, 1, tiled=True)[0]
    sites = lax.all_gather(sites_here, "slab_3", axis=0, tiled=True)
    top, bottom = sites[1:2], sites[0:1]
    even = jnp.concatenate([own, jnp.where(parity == 0, top, bottom)], axis=0)
    odd = jnp.concatenate([own, jnp.where(parity == 0, bottom, top)], axis=0)
    even, odd = exchange(even, inside), exchange(odd, across)
    one, two, part = call(
        functools.partial(before_kernel, True),
        (PLANES, PLANES, shape(1, 8, 128)), [VMEM] * 3, "before_first",
    )(base, own, sites)
    parts = [part]
    ones, twos = [], [own]
    one, two, edge, edge_sites = call(
        functools.partial(after_kernel, True, False),
        (PLANES,) * 4, [SMEM] + [VMEM] * 7, "after_first",
    )(side, base, even, odd, own, sites, one, two)
    swapped = None
    for step in range(1, 4):
        ones.append(one)
        twos.append(two)
        even, odd = exchange(two, inside), exchange(two, across)
        one, two, part = call(
            functools.partial(before_kernel, False),
            (PLANES, PLANES, shape(4, 8, 128)), [VMEM] * 5, "before",
        )(base, twos[-1], sites, ones[-1], twos[-2])
        parts.append(part)
        if step == 2:
            swapped = exchange(
                call(swap_kernel, shape(3, 256, 256), [SMEM] + [VMEM] * 3, "swap")(
                    side, ones[0], twos[1], ones[1]
                ),
                partner,
            )
        operands = (side, base, even, odd, twos[-1], sites, one, two, edge_sites, edge)
        if step < 3:
            one, two, edge = call(
                functools.partial(after_kernel, False, False),
                (PLANES,) * 3, [SMEM] + [VMEM] * 9, "after",
            )(*operands)
        else:
            row = call(
                functools.partial(after_kernel, False, True),
                shape(1, 128), [SMEM] + [VMEM] * 13, "after_last",
            )(*operands, *parts)
    rows = gathered(row, STAGES[0], 32)
    rows = gathered(jnp.sum(rows, axis=0, keepdims=True), STAGES[1], 16)
    field, diag, offd, moments, good = call(
        finish_kernel,
        (
            shape(2, 1, 256, 256), shape(2, 8), shape(2, 7), shape(2, 6),
            jax.ShapeDtypeStruct((1,), jnp.int32),
        ),
        [SMEM] + [VMEM] * 7, "finish",
    )(side, base, rows, start_vectors, ones[0], twos[1], ones[1], swapped)

    def accept(field, diag, offd, moments, *_):
        return (field, diag, offd, moments)

    def redo(field, diag, offd, moments, *inputs):
        return stepwise(*inputs)

    return lax.cond(
        good[0] == 1, accept, redo,
        field, diag, offd, moments, start_vectors, levels, energies,
    )


def solution(mesh):
    split = Mesh(mesh.devices.reshape(8, 4, 8, 2), SLAB)
    in_specs = (P(None, SLAB, None, None), P(SLAB, None, None), P())
    out_specs = (P(None, SLAB, None, None), P(), P(), P())
    return jax.shard_map(
        shards, mesh=split, in_specs=in_specs, out_specs=out_specs, check_vma=False
    )
```

```python
import functools

import jax
import jax.numpy as jnp
from jax import lax
from jax.experimental import pallas as pl
from jax.experimental.pallas import tpu as pltpu
from jax.sharding import Mesh
from jax.sharding import PartitionSpec as P

LANCZOS = 8
SLAB = ("slab_0", "slab_1", "slab_2", "slab_3")
STAGES = (("slab_1", "slab_2"), ("slab_0", "slab_3"))
ROWS = 32
NUDGE = 1e-3
ROUNDING = 2e-7
TOLERANCE = 1e-4
VMEM = pl.BlockSpec(memory_space=pltpu.VMEM)
SMEM = pl.BlockSpec(memory_space=pltpu.SMEM)
PARAMS = pltpu.CompilerParams(vmem_limit_bytes=24 * 1024 * 1024)


def from_behind(block, axis, distance):
    devices = range(lax.axis_size(axis))
    route = [((i - distance) % len(devices), i) for i in devices]
    return lax.ppermute(block, axis, route)


def one_axis_at_a_time(value, axes):
    for axis in axes:
        value = lax.psum(value, axis)
    return value


def inner(first, second):
    return jnp.sum(first * second, axis=(1, 2, 3))


def expand(values):
    return values[:, None, None, None]


def hamiltonian(field, onsite):
    below = from_behind(field, SLAB, 1)
    above = from_behind(field, SLAB, -1)
    beside = jnp.roll(field, 1, 2) + jnp.roll(field, -1, 2)
    beside = beside + jnp.roll(field, 1, 3) + jnp.roll(field, -1, 3)
    return onsite[None] * field - (beside + below + above)


def stepwise(start_vectors, levels, energies):
    level_ids = lax.broadcasted_iota(jnp.int32, (energies.shape[0], 1, 1, 1), 0)
    onsite = jnp.sum(
        jnp.where(levels[None] == level_ids, energies[:, None, None, None], 0.0), axis=0
    )
    vec_count = start_vectors.shape[0]
    norm0 = one_axis_at_a_time(inner(start_vectors, start_vectors), SLAB)

    def lanczos(state, step):
        vector, previous, beta_prev = state
        work = hamiltonian(vector, onsite) - expand(beta_prev) * previous
        alpha = one_axis_at_a_time(inner(vector, work), SLAB)
        work = work - expand(alpha) * vector
        beta = jnp.sqrt(one_axis_at_a_time(inner(work, work), SLAB))
        return (work / expand(beta), vector, beta), (alpha, beta)

    vector = start_vectors / expand(jnp.sqrt(norm0))
    _, (alphas, betas) = lax.scan(
        lanczos,
        (vector, jnp.zeros_like(vector), jnp.zeros((vec_count,), jnp.float32)),
        None,
        length=LANCZOS,
    )
    diag = alphas.T
    offd = betas[: LANCZOS - 1].T
    zero_col = jnp.zeros((vec_count, 1), jnp.float32)
    left = jnp.concatenate([zero_col, offd], axis=1)
    right = jnp.concatenate([offd, zero_col], axis=1)
    emin = jnp.min(diag - left - right, axis=1)
    emax = jnp.max(diag + left + right, axis=1)
    center = expand((emax + emin) * 0.5)
    half = expand(0.55 * (emax - emin))

    def scaled(field):
        return (hamiltonian(field, onsite) - center * field) / half

    term1 = scaled(start_vectors)
    term2 = 2.0 * scaled(term1) - start_vectors
    term3 = 2.0 * scaled(term2) - term1
    local = jnp.stack(
        [
            inner(start_vectors, term1),
            inner(start_vectors, term2),
            inner(start_vectors, term3),
            inner(term2, term2),
            inner(term3, term2),
            inner(term3, term3),
        ],
        axis=0,
    )
    sums = one_axis_at_a_time(local, SLAB)
    moments = (
        jnp.stack(
            [
                sums[0],
                sums[1],
                sums[2],
                2.0 * sums[3] - norm0,
                2.0 * sums[4] - sums[0],
                2.0 * sums[5] - norm0,
            ],
            axis=1,
        )
        / norm0[:, None]
    )
    return (term3, diag, offd, moments)


def shape(*dims):
    return jax.ShapeDtypeStruct(dims, jnp.float32)


PLANES = shape(2, 256, 256)
CHUNKS = 256 // ROWS
PAIR_COST = pl.CostEstimate(flops=4_000_000, bytes_accessed=4_000_000, transcendentals=0)


def call(kernel, out_shape, in_specs, name, scratch=()):
    return pl.pallas_call(
        kernel,
        out_shape=out_shape,
        in_specs=in_specs,
        out_specs=jax.tree.map(
            lambda leaf: SMEM if leaf.dtype == jnp.int32 else VMEM, out_shape
        ),
        scratch_shapes=scratch,
        compiler_params=PARAMS,
        cost_estimate=PAIR_COST,
        name=name,
    )


def onsite_kernel(energies_ref, levels_ref, start, out_ref, send_ref, base_ref):
    count = energies_ref.shape[1]
    values = [
        jnp.broadcast_to(energies_ref[0:1, index : index + 1], (1, 256))
        for index in range(count)
    ]
    mean = functools.reduce(jnp.add, values) * (1.0 / count)
    spread = functools.reduce(jnp.add, [jnp.square(v - mean) for v in values])
    scale = 1.05 * jnp.sqrt(6.0 + spread * (1.0 / count))
    inverse = 1.0 / scale
    base_ref[0:1] = mean
    base_ref[1:2] = inverse
    base_ref[2:3] = scale
    base_ref[3:4] = inverse * inverse
    values = [(v - mean) * inverse for v in values]
    other = 1 - lax.axis_index(SLAB[3])

    def rows_of(chunk, carry):
        rows = pl.ds(chunk * ROWS, ROWS)
        level = levels_ref[0, rows]
        value = jnp.zeros(level.shape, jnp.float32)
        for index in range(count):
            value = jnp.where(level == index, values[index], value)
        out_ref[rows] = value
        send_ref[1, rows] = value
        send_ref[0, rows] = start[other, 0, rows]
        return carry

    lax.fori_loop(0, CHUNKS, rows_of, 0)


def assemble_kernel(start, sites_here, received, own_ref, sites_ref):
    here = lax.axis_index(SLAB[3])

    def body(chunk, carry):
        rows = pl.ds(chunk * ROWS, ROWS)
        own_ref[here, rows] = start[here, 0, rows]
        own_ref[1 - here, rows] = received[0, rows]
        sites_ref[here, rows] = sites_here[rows]
        sites_ref[1 - here, rows] = received[1, rows]
        return carry

    chunks(body, 0)


def join_kernel(mine, theirs, out_ref):
    here = lax.axis_index(SLAB[3])

    def body(chunk, carry):
        rows = pl.ds(chunk * ROWS, ROWS)
        out_ref[here, rows] = mine[rows]
        out_ref[1 - here, rows] = theirs[rows]
        return carry

    chunks(body, 0)


def in_plane(plane, chunk):
    rows = pl.ds(chunk * ROWS, ROWS)
    before = pl.ds(pl.multiple_of((chunk * ROWS + 248) % 256, 8), 8)
    after = pl.ds(pl.multiple_of((chunk * ROWS + ROWS) % 256, 8), 8)
    middle = plane[rows]
    tall = jnp.concatenate([plane[before], middle, plane[after]], axis=0)
    beside = pltpu.roll(tall, 1, 0)[8 : 8 + ROWS]
    beside = beside + pltpu.roll(tall, ROWS + 15, 0)[8 : 8 + ROWS]
    return beside + (pltpu.roll(middle, 1, 1) + pltpu.roll(middle, 255, 1)), middle


def folded(values):
    total = values[:, :128] + values[:, 128:]
    return jnp.sum(total.reshape(ROWS // 8, 8, 128), axis=0)


def chunks(body, count):
    zero = jnp.zeros((8, 128), jnp.float32)
    return lax.fori_loop(0, CHUNKS, body, (zero,) * count)


def before_kernel(first, base_ref, own, sites, *refs):
    if first:
        first_ref, second_ref, sums = refs
    else:
        prior, older, first_ref, second_ref, sums = refs
    inverse = base_ref[1:2]

    def once(chunk, carry):
        rows = pl.ds(chunk * ROWS, ROWS)
        for j in range(2):
            beside, middle = in_plane(own.at[j], chunk)
            value = sites[j, rows] * middle - inverse * (beside + own[1 - j, rows])
            if first:
                carry = (carry[0] + folded(middle * middle),)
            else:
                last = prior[j, rows]
                value = value - last
                carry = (
                    carry[0] + folded(last * older[j, rows]),
                    carry[1] + folded(last * last),
                    carry[2] + folded(middle * last),
                    carry[3] + folded(middle * middle),
                )
            first_ref[j, rows] = value
        return carry

    totals = chunks(once, 1 if first else 4)

    def twice(chunk, carry):
        rows = pl.ds(chunk * ROWS, ROWS)
        for j in range(2):
            beside, middle = in_plane(first_ref.at[j], chunk)
            beside = beside + first_ref[1 - j, rows]
            second_ref[j, rows] = sites[j, rows] * middle - inverse * beside - own[j, rows]
        return carry

    chunks(twice, 0)
    for index, total in enumerate(totals):
        sums[index] = total


def after_kernel(first, last, base_ref, even_ref, odd_ref, own, sites, one, two, *refs):
    refs = list(refs)
    edge_sites = refs.pop(0)
    if not first:
        edge_prior = refs.pop(0)
    if last:
        parts, row_ref = refs[:4], refs[4]
    else:
        new_one, new_two, new_edge = refs
    inverse, inverse2 = base_ref[1:2], base_ref[3:4]

    def run(low, high):
        def body(chunk, carry):
            rows = pl.ds(chunk * ROWS, ROWS)
            near, far = (low.at[1], high.at[0]), (low.at[0], high.at[1])
            found = [in_plane(plane, chunk) for plane in near]
            for j in range(2):
                beside, middle = found[j]
                site = edge_sites[j, rows]
                mine = own[j, rows]
                edge = site * middle - inverse * (beside + far[j][rows] + mine)
                if not first:
                    edge = edge - edge_prior[j, rows]
                value = one[j, rows] - inverse * middle
                new = two[j, rows] - inverse * (sites[j, rows] * middle + edge)
                new = new + inverse2 * (beside + found[1 - j][1])
                if last:
                    carry = (
                        carry[0] + folded(value * mine),
                        carry[1] + folded(value * value),
                        carry[2] + folded(new * value),
                    )
                else:
                    new_one[j, rows] = value
                    new_two[j, rows] = new
                    new_edge[j, rows] = edge
            return carry

        totals = chunks(body, 3 if last else 0)
        if last:
            pack(parts, totals, row_ref)

    parity = lax.axis_index(SLAB[2]) % 2

    @pl.when(parity == 0)
    def _():
        run(odd_ref, even_ref)

    @pl.when(parity == 1)
    def _():
        run(even_ref, odd_ref)


def pack(parts, totals, row_ref):
    entries = [(0, parts[0][0])]
    for index in range(3):
        places = (8 + 2 * index, 2 * index + 1, 9 + 2 * index, 2 * index + 2)
        entries += [(place, parts[index + 1][k]) for k, place in enumerate(places)]
    entries += list(zip((14, 7, 15), totals))
    lane = lax.broadcasted_iota(jnp.int32, (1, 128), 1)
    row = jnp.zeros((1, 128), jnp.float32)
    for place, value in entries:
        total = jnp.sum(jnp.sum(value, axis=0, keepdims=True), axis=1, keepdims=True)
        row = jnp.where(lane == place, total, row)
    row_ref[...] = row


def swap_kernel(p1, p2, p3, out_ref):
    other = 1 - lax.axis_index(SLAB[3])

    def body(chunk, carry):
        rows = pl.ds(chunk * ROWS, ROWS)
        for index, ref in enumerate((p1, p2, p3)):
            out_ref[index, rows] = ref[other, rows]
        return carry

    chunks(body, 0)


def finish_kernel(
    base_ref, rows_ref, start, p1, p2, p3, swapped,
    field_ref, diag_ref, offd_ref, moments_ref, good_ref,
):
    shift, scale = base_ref[0:1, :128], base_ref[2:3, :128]
    lane = lax.broadcasted_iota(jnp.int32, (2, 128), 1)
    rows = rows_ref[...]
    sub = lax.broadcasted_iota(jnp.int32, rows.shape, 0)
    even = jnp.sum(jnp.where(sub % 2 == 0, rows, 0.0), axis=0, keepdims=True)
    odd = jnp.sum(jnp.where(sub % 2 == 1, rows, 0.0), axis=0, keepdims=True)
    total = jnp.concatenate([even, odd], axis=0)

    def column(index):
        return jnp.broadcast_to(total[:, index : index + 1], (2, 128))

    plain = [column(index) for index in range(8)]
    largest = [jnp.maximum(plain[k], plain[min(k + 1, 7)]) for k in range(8)]
    square = [
        plain[k] + jnp.where(lane == k + 1, NUDGE * plain[k], 0.0) for k in range(8)
    ]
    cross = [
        column(8 + k) + jnp.where(lane == k + 9, NUDGE * largest[k], 0.0) for k in range(8)
    ]
    moment = []
    for k in range(8):
        moment.append(square[k] - square[k - 1] if k else square[k])
        moment.append(cross[k] - cross[k - 1] if k else cross[k])
    norm0 = moment[0]
    sigma = [value / norm0 for value in moment]
    normal = list(sigma)
    zero = jnp.zeros_like(norm0)
    older = [zero] * len(sigma)
    alphas, betas = [], []
    weight = zero
    for k in range(LANCZOS):
        size = len(sigma)
        pushed = [
            (sigma[l + 1] + sigma[l - 1]) if l else sigma[1] for l in range(size - 1)
        ]
        ratio = (pushed[k] - weight * older[k]) / sigma[k]
        alphas.append(ratio)
        if k < LANCZOS - 1:
            fresh = [
                pushed[l] - ratio * sigma[l] - weight * older[l] for l in range(size - 1)
            ]
            weight = fresh[k + 1] / sigma[k]
            betas.append(jnp.sqrt(weight))
            older, sigma = sigma, fresh
    alphas = [scale * value + shift for value in alphas]
    betas = [scale * value for value in betas]

    def spread(values):
        error, norm = zero, zero
        for value in values:
            exact = jnp.broadcast_to(value[:, :1], value.shape)
            error = error + jnp.square(
                jnp.broadcast_to(
                    jnp.sum(jnp.abs(value - exact), axis=1, keepdims=True), value.shape
                )
            )
            norm = norm + jnp.square(exact)
        error = jnp.sum(error, axis=0, keepdims=True)
        norm = jnp.sum(norm, axis=0, keepdims=True)
        allowed = TOLERANCE * NUDGE / ROUNDING
        return jnp.where(error <= allowed * allowed * norm, 1, 0)

    fits = jnp.minimum(spread(alphas), spread(betas))
    good_ref[0] = jnp.min(fits)

    lows, highs = [], []
    for k in range(LANCZOS):
        left = betas[k - 1] if k else zero
        right = betas[k] if k < LANCZOS - 1 else zero
        lows.append(alphas[k] - left - right)
        highs.append(alphas[k] + left + right)
    emin = functools.reduce(jnp.minimum, lows)
    emax = functools.reduce(jnp.maximum, highs)
    center = (emax + emin) * 0.5
    half = 0.55 * (emax - emin)
    offset = (shift - center) / half
    factor = scale / half

    def apply(coefs):
        out = []
        for l in range(len(coefs) + 1):
            value = zero
            if l < len(coefs):
                value = value + offset * coefs[l]
            if l + 1 < len(coefs):
                value = value + factor * coefs[l + 1]
            if l:
                value = value + factor * coefs[l - 1]
            out.append(value)
        return out

    terms = [[zero + 1.0]]
    terms.append(apply(terms[0]))
    for m in range(2, 7):
        nxt = apply(terms[-1])
        old = terms[-2]
        terms.append(
            [2.0 * v - (old[l] if l < len(old) else zero) for l, v in enumerate(nxt)]
        )
    diag, offd, out = zero, zero, zero
    for k in range(LANCZOS):
        diag = jnp.where(lane == k, jnp.broadcast_to(alphas[k][:, :1], lane.shape), diag)
        if k < LANCZOS - 1:
            offd = jnp.where(lane == k, jnp.broadcast_to(betas[k][:, :1], lane.shape), offd)
    for m in range(1, 7):
        value = functools.reduce(
            jnp.add, [c * normal[l] for l, c in enumerate(terms[m])]
        )
        out = jnp.where(lane == m - 1, jnp.broadcast_to(value[:, :1], lane.shape), out)
    diag_ref[...] = diag[:, :8]
    offd_ref[...] = offd[:, :7]
    moments_ref[...] = out[:, :6]

    here = lax.axis_index(SLAB[3])
    wide = [
        jnp.concatenate([jnp.broadcast_to(terms[3][l][:, :1], lane.shape)] * 2, axis=1)
        for l in range(4)
    ]
    mine = [jnp.where(here == 1, w[1:2], w[0:1]) for w in wide]
    other = [jnp.where(here == 1, w[0:1], w[1:2]) for w in wide]

    def combine(chunk, carry):
        at = pl.ds(chunk * ROWS, ROWS)
        value = mine[0] * start[here, 0, at]
        for l, ref in enumerate((p1, p2, p3)):
            value = value + mine[l + 1] * ref[here, at]
        field_ref[here, 0, at] = value
        value = other[0] * start[1 - here, 0, at]
        for l in range(3):
            value = value + other[l + 1] * swapped[l, at]
        field_ref[1 - here, 0, at] = value
        return carry

    chunks(combine, 0)


def gathered(row, axes, count):
    copies = jnp.broadcast_to(row[None], (count,) + row.shape)
    return lax.all_to_all(copies, axes, 0, 0, tiled=True).reshape(count, 128)


def exchange(block, route):
    return lax.ppermute(block, SLAB, route)


def shards(start_vectors, levels, energies):
    devices = 512
    inside = [(i, i ^ 2) for i in range(devices)]
    across = [(i, (((i + 2) ^ 2) - 2) % devices) for i in range(devices)]
    partner = [(i, i ^ 1) for i in range(devices)]
    adjacent = [(i, (((i + 1) ^ 1) - 1) % devices) for i in range(devices)]

    sites_here, send, base = call(
        onsite_kernel, (shape(256, 256), PLANES, shape(8, 256)),
        [VMEM] * 3, "onsite",
    )(energies.reshape(1, -1), levels, start_vectors)
    beyond = exchange(sites_here, adjacent)
    own, sites = call(
        assemble_kernel, (PLANES, PLANES), [VMEM] * 3, "assemble"
    )(start_vectors, sites_here, exchange(send, partner))
    even, odd = exchange(own, inside), exchange(own, across)
    one, two, part = call(
        functools.partial(before_kernel, True),
        (PLANES, PLANES, shape(1, 8, 128)), [VMEM] * 3, "before_first",
    )(base, own, sites)
    beyond, part = lax.optimization_barrier((beyond, part))
    edge_sites = call(join_kernel, PLANES, [VMEM] * 2, "join")(
        beyond, exchange(beyond, partner)
    )
    parts = [part]
    ones, twos = [], [own]
    one, two, edge = call(
        functools.partial(after_kernel, True, False),
        (PLANES,) * 3, [VMEM] * 8, "after_first",
    )(base, even, odd, own, sites, one, two, edge_sites)
    swapped = None
    for step in range(1, 4):
        ones.append(one)
        twos.append(two)
        even, odd = exchange(two, inside), exchange(two, across)
        one, two, part = call(
            functools.partial(before_kernel, False),
            (PLANES, PLANES, shape(4, 8, 128)), [VMEM] * 5, "before",
        )(base, twos[-1], sites, ones[-1], twos[-2])
        parts.append(part)
        if step == 2:
            swapped = exchange(
                call(swap_kernel, shape(3, 256, 256), [VMEM] * 3, "swap")(
                    ones[0], twos[1], ones[1]
                ),
                partner,
            )
        operands = (base, even, odd, twos[-1], sites, one, two, edge_sites, edge)
        if step < 3:
            one, two, edge = call(
                functools.partial(after_kernel, False, False),
                (PLANES,) * 3, [VMEM] * 9, "after",
            )(*operands)
        else:
            row = call(
                functools.partial(after_kernel, False, True),
                shape(1, 128), [VMEM] * 13, "after_last",
            )(*operands, *parts)
    rows = gathered(row, STAGES[0], 32)
    rows = gathered(jnp.sum(rows, axis=0, keepdims=True), STAGES[1], 16)
    field, diag, offd, moments, good = call(
        finish_kernel,
        (
            shape(2, 1, 256, 256), shape(2, 8), shape(2, 7), shape(2, 6),
            jax.ShapeDtypeStruct((1,), jnp.int32),
        ),
        [VMEM] * 7, "finish",
    )(base, rows, start_vectors, ones[0], twos[1], ones[1], swapped)

    def accept(field, diag, offd, moments, *_):
        return (field, diag, offd, moments)

    def redo(field, diag, offd, moments, *inputs):
        return stepwise(*inputs)

    return lax.cond(
        good[0] == 1, accept, redo,
        field, diag, offd, moments, start_vectors, levels, energies,
    )


def solution(mesh):
    split = Mesh(mesh.devices.reshape(8, 4, 8, 2), SLAB)
    in_specs = (P(None, SLAB, None, None), P(SLAB, None, None), P())
    out_specs = (P(None, SLAB, None, None), P(), P(), P())
    return jax.shard_map(
        shards, mesh=split, in_specs=in_specs, out_specs=out_specs, check_vma=False
    )
```

```python
import functools

import jax
import jax.numpy as jnp
from jax import lax
from jax.experimental import pallas as pl
from jax.experimental.pallas import tpu as pltpu
from jax.sharding import Mesh
from jax.sharding import PartitionSpec as P

LANCZOS = 8
SLAB = ("slab_0", "slab_1", "slab_2", "slab_3")
STAGES = (("slab_1", "slab_2"), ("slab_0", "slab_3"))
ROWS = 64
NUDGE = 1e-3
ROUNDING = 2e-7
TOLERANCE = 1e-4
VMEM = pl.BlockSpec(memory_space=pltpu.VMEM)
PARAMS = pltpu.CompilerParams(vmem_limit_bytes=24 * 1024 * 1024)


def from_behind(block, axis, distance):
    devices = range(lax.axis_size(axis))
    route = [((i - distance) % len(devices), i) for i in devices]
    return lax.ppermute(block, axis, route)


def one_axis_at_a_time(value, axes):
    for axis in axes:
        value = lax.psum(value, axis)
    return value


def inner(first, second):
    return jnp.sum(first * second, axis=(1, 2, 3))


def expand(values):
    return values[:, None, None, None]


def hamiltonian(field, onsite):
    below = from_behind(field, SLAB, 1)
    above = from_behind(field, SLAB, -1)
    beside = jnp.roll(field, 1, 2) + jnp.roll(field, -1, 2)
    beside = beside + jnp.roll(field, 1, 3) + jnp.roll(field, -1, 3)
    return onsite[None] * field - (beside + below + above)


def stepwise(start_vectors, levels, energies):
    level_ids = lax.broadcasted_iota(jnp.int32, (energies.shape[0], 1, 1, 1), 0)
    onsite = jnp.sum(
        jnp.where(levels[None] == level_ids, energies[:, None, None, None], 0.0), axis=0
    )
    vec_count = start_vectors.shape[0]
    norm0 = one_axis_at_a_time(inner(start_vectors, start_vectors), SLAB)

    def lanczos(state, step):
        vector, previous, beta_prev = state
        work = hamiltonian(vector, onsite) - expand(beta_prev) * previous
        alpha = one_axis_at_a_time(inner(vector, work), SLAB)
        work = work - expand(alpha) * vector
        beta = jnp.sqrt(one_axis_at_a_time(inner(work, work), SLAB))
        return (work / expand(beta), vector, beta), (alpha, beta)

    vector = start_vectors / expand(jnp.sqrt(norm0))
    _, (alphas, betas) = lax.scan(
        lanczos,
        (vector, jnp.zeros_like(vector), jnp.zeros((vec_count,), jnp.float32)),
        None,
        length=LANCZOS,
    )
    diag = alphas.T
    offd = betas[: LANCZOS - 1].T
    zero_col = jnp.zeros((vec_count, 1), jnp.float32)
    left = jnp.concatenate([zero_col, offd], axis=1)
    right = jnp.concatenate([offd, zero_col], axis=1)
    emin = jnp.min(diag - left - right, axis=1)
    emax = jnp.max(diag + left + right, axis=1)
    center = expand((emax + emin) * 0.5)
    half = expand(0.55 * (emax - emin))

    def scaled(field):
        return (hamiltonian(field, onsite) - center * field) / half

    term1 = scaled(start_vectors)
    term2 = 2.0 * scaled(term1) - start_vectors
    term3 = 2.0 * scaled(term2) - term1
    local = jnp.stack(
        [
            inner(start_vectors, term1),
            inner(start_vectors, term2),
            inner(start_vectors, term3),
            inner(term2, term2),
            inner(term3, term2),
            inner(term3, term3),
        ],
        axis=0,
    )
    sums = one_axis_at_a_time(local, SLAB)
    moments = (
        jnp.stack(
            [
                sums[0],
                sums[1],
                sums[2],
                2.0 * sums[3] - norm0,
                2.0 * sums[4] - sums[0],
                2.0 * sums[5] - norm0,
            ],
            axis=1,
        )
        / norm0[:, None]
    )
    return (term3, diag, offd, moments)


def shape(*dims):
    return jax.ShapeDtypeStruct(dims, jnp.float32)


PLANES = shape(2, 256, 256)
CHUNKS = 256 // ROWS
PAIR_COST = pl.CostEstimate(flops=4_000_000, bytes_accessed=4_000_000, transcendentals=0)


def call(kernel, out_shape, in_specs, name, scratch=()):
    return pl.pallas_call(
        kernel,
        out_shape=out_shape,
        in_specs=in_specs,
        out_specs=jax.tree.map(lambda leaf: VMEM, out_shape),
        scratch_shapes=scratch,
        compiler_params=PARAMS,
        cost_estimate=PAIR_COST,
        name=name,
    )


def sides():
    parity = lax.axis_index(SLAB[2]) % 2
    core = lax.axis_index(SLAB[3])
    return parity, core, jnp.where(core == parity, 0, 1)


def onsite_kernel(energies_ref, levels_ref, start, out_ref, send_ref, base_ref):
    count = energies_ref.shape[1]
    values = [
        jnp.broadcast_to(energies_ref[0:1, index : index + 1], (1, 256))
        for index in range(count)
    ]
    mean = functools.reduce(jnp.add, values) * (1.0 / count)
    spread = functools.reduce(jnp.add, [jnp.square(v - mean) for v in values])
    scale = 1.05 * jnp.sqrt(6.0 + spread * (1.0 / count))
    inverse = 1.0 / scale
    base_ref[0:1] = mean
    base_ref[1:2] = inverse
    base_ref[2:3] = scale
    values = [(v - mean) * inverse for v in values]
    core = lax.axis_index(SLAB[3])

    def rows_of(chunk, carry):
        rows = pl.ds(chunk * ROWS, ROWS)
        level = levels_ref[0, rows]
        value = jnp.zeros(level.shape, jnp.float32)
        for index in range(count):
            value = jnp.where(level == index, values[index], value)
        out_ref[0, rows] = value
        out_ref[1, rows] = start[core, 0, rows]
        send_ref[1, rows] = value
        send_ref[0, rows] = start[1 - core, 0, rows]
        return carry

    lax.fori_loop(0, CHUNKS, rows_of, 0)


def in_plane(plane, chunk):
    rows = pl.ds(chunk * ROWS, ROWS)
    before = pl.ds(pl.multiple_of((chunk * ROWS + 248) % 256, 8), 8)
    after = pl.ds(pl.multiple_of((chunk * ROWS + ROWS) % 256, 8), 8)
    middle = plane[rows]
    tall = jnp.concatenate([plane[before], middle, plane[after]], axis=0)
    beside = pltpu.roll(tall, 1, 0)[8 : 8 + ROWS]
    beside = beside + pltpu.roll(tall, ROWS + 15, 0)[8 : 8 + ROWS]
    return beside + (pltpu.roll(middle, 1, 1) + pltpu.roll(middle, 255, 1)), middle


def folded(values):
    total = values[:, :128] + values[:, 128:]
    return jnp.sum(total.reshape(ROWS // 8, 8, 128), axis=0)


def chunks(body, count):
    zero = jnp.zeros((8, 128), jnp.float32)
    return lax.fori_loop(0, CHUNKS, body, (zero,) * count)


def partial(fields, sites, prior, inverse):
    def body(chunk, carry):
        rows = pl.ds(chunk * ROWS, ROWS)
        for s in range(2):
            beside, middle = in_plane(fields[s].at[0], chunk)
            value = sites[s, rows] * middle - inverse * (beside + fields[1 - s][0, rows])
            if prior is not None:
                value = value - prior[s, rows]
            fields[s][1, rows] = value
        return carry

    chunks(body, 0)


def assemble_kernel(base_ref, here_ref, received, across_ref, inside_ref, sites_ref):
    mine = sides()[2]

    def body(chunk, carry):
        rows = pl.ds(chunk * ROWS, ROWS)
        kept, taken = here_ref[1, rows], received[0, rows]
        across_ref[0, rows] = jnp.where(mine == 0, kept, taken)
        inside_ref[0, rows] = jnp.where(mine == 0, taken, kept)
        sites_ref[mine, rows] = here_ref[0, rows]
        sites_ref[1 - mine, rows] = received[1, rows]
        return carry

    chunks(body, 0)
    partial((across_ref, inside_ref), sites_ref, None, base_ref[1:2])


def round_kernel(last, base_ref, across, inside, from_across, from_inside, sites, *refs):
    if last:
        parts, row_ref, one = refs[:3], refs[3], refs[4]
    else:
        one, new_across, new_inside = refs
        fields = (new_across, new_inside)
    own, got = (across, inside), (from_across, from_inside)
    inverse = base_ref[1:2]

    def first(chunk, carry):
        rows = pl.ds(chunk * ROWS, ROWS)
        for s in range(2):
            value = own[s][1, rows] - inverse * got[s][0, rows]
            one[s, rows] = value
            if last:
                carry = (
                    carry[0] + folded(value * own[s][0, rows]),
                    carry[1] + folded(value * value),
                )
        return carry

    totals = chunks(first, 2 if last else 0)

    def second(chunk, carry):
        rows = pl.ds(chunk * ROWS, ROWS)
        for s in range(2):
            beside, middle = in_plane(one.at[s], chunk)
            field = own[s][0, rows]
            edge = got[s][1, rows] - inverse * field
            beside = beside + (one[1 - s, rows] + edge)
            value = sites[s, rows] * middle - inverse * beside - field
            if last:
                carry = (carry[0] + folded(value * middle),)
            else:
                fields[s][0, rows] = value
        return carry

    final = chunks(second, 1 if last else 0)
    if last:
        pack(parts, tuple(totals) + tuple(final), row_ref)
    else:
        partial(fields, sites, one, inverse)


def sums_kernel(first, across, inside, one, new_across, new_inside, sums):
    old, new = (across, inside), (new_across, new_inside)

    def body(chunk, carry):
        rows = pl.ds(chunk * ROWS, ROWS)
        for s in range(2):
            field, value, later = old[s][0, rows], one[s, rows], new[s][0, rows]
            terms = [value * field, value * value, later * value, later * later]
            if first:
                terms.append(field * field)
            carry = tuple(c + folded(t) for c, t in zip(carry, terms))
        return carry

    for index, total in enumerate(chunks(body, 5 if first else 4)):
        sums[index] = total


def pack(parts, totals, row_ref):
    entries = [(0, parts[0][4])]
    for index in range(3):
        places = (8 + 2 * index, 2 * index + 1, 9 + 2 * index, 2 * index + 2)
        entries += [(place, parts[index][k]) for k, place in enumerate(places)]
    entries += list(zip((14, 7, 15), totals))
    lane = lax.broadcasted_iota(jnp.int32, (1, 128), 1)
    row = jnp.zeros((1, 128), jnp.float32)
    for place, value in entries:
        total = jnp.sum(jnp.sum(value, axis=0, keepdims=True), axis=1, keepdims=True)
        row = jnp.where(lane == place, total, row)
    row_ref[...] = jnp.broadcast_to(row, row_ref.shape)


def total_kernel(rows_ref, out_ref):
    total = jnp.sum(rows_ref[...], axis=0, keepdims=True)
    out_ref[...] = jnp.broadcast_to(total, out_ref.shape)


def swap_kernel(p0_across, p0_inside, p1, p2_across, p2_inside, p3, out_ref):
    other = 1 - sides()[2]

    def body(chunk, carry):
        rows = pl.ds(chunk * ROWS, ROWS)
        out_ref[0, rows] = jnp.where(other == 0, p0_across[0, rows], p0_inside[0, rows])
        out_ref[1, rows] = p1[other, rows]
        out_ref[2, rows] = jnp.where(other == 0, p2_across[0, rows], p2_inside[0, rows])
        out_ref[3, rows] = p3[other, rows]
        return carry

    chunks(body, 0)


def finish_kernel(
    base_ref, rows_ref, p0_across, p0_inside, p1, p2_across, p2_inside, p3, swapped,
    field_ref, diag_ref, offd_ref, moments_ref, good_ref,
):
    shift, scale = base_ref[0:1, :128], base_ref[2:3, :128]
    lane = lax.broadcasted_iota(jnp.int32, (2, 128), 1)
    rows = rows_ref[...]
    sub = lax.broadcasted_iota(jnp.int32, rows.shape, 0)
    even = jnp.sum(jnp.where(sub % 2 == 0, rows, 0.0), axis=0, keepdims=True)
    odd = jnp.sum(jnp.where(sub % 2 == 1, rows, 0.0), axis=0, keepdims=True)
    total = jnp.concatenate([even, odd], axis=0)

    def column(index):
        return jnp.broadcast_to(total[:, index : index + 1], (2, 128))

    plain = [column(index) for index in range(8)]
    largest = [jnp.maximum(plain[k], plain[min(k + 1, 7)]) for k in range(8)]
    square = [
        plain[k] + jnp.where(lane == k + 1, NUDGE * plain[k], 0.0) for k in range(8)
    ]
    cross = [
        column(8 + k) + jnp.where(lane == k + 9, NUDGE * largest[k], 0.0) for k in range(8)
    ]
    moment = []
    for k in range(8):
        moment.append(square[k] - square[k - 1] if k else square[k])
        moment.append(cross[k] - cross[k - 1] if k else cross[k])
    norm0 = moment[0]
    sigma = [value / norm0 for value in moment]
    normal = list(sigma)
    zero = jnp.zeros_like(norm0)
    older = [zero] * len(sigma)
    alphas, betas = [], []
    weight = zero
    for k in range(LANCZOS):
        size = len(sigma)
        pushed = [
            (sigma[l + 1] + sigma[l - 1]) if l else sigma[1] for l in range(size - 1)
        ]
        ratio = (pushed[k] - weight * older[k]) / sigma[k]
        alphas.append(ratio)
        if k < LANCZOS - 1:
            fresh = [
                pushed[l] - ratio * sigma[l] - weight * older[l] for l in range(size - 1)
            ]
            weight = fresh[k + 1] / sigma[k]
            betas.append(jnp.sqrt(weight))
            older, sigma = sigma, fresh
    alphas = [scale * value + shift for value in alphas]
    betas = [scale * value for value in betas]

    def spread(values):
        error, norm = zero, zero
        for value in values:
            exact = jnp.broadcast_to(value[:, :1], value.shape)
            error = error + jnp.square(
                jnp.broadcast_to(
                    jnp.sum(jnp.abs(value - exact), axis=1, keepdims=True), value.shape
                )
            )
            norm = norm + jnp.square(exact)
        error = jnp.sum(error, axis=0, keepdims=True)
        norm = jnp.sum(norm, axis=0, keepdims=True)
        allowed = TOLERANCE * NUDGE / ROUNDING
        return jnp.where(error <= allowed * allowed * norm, 1, 0)

    fits = jnp.minimum(spread(alphas), spread(betas))
    good_ref[...] = jnp.broadcast_to(fits[0:1], good_ref.shape)

    lows, highs = [], []
    for k in range(LANCZOS):
        left = betas[k - 1] if k else zero
        right = betas[k] if k < LANCZOS - 1 else zero
        lows.append(alphas[k] - left - right)
        highs.append(alphas[k] + left + right)
    emin = functools.reduce(jnp.minimum, lows)
    emax = functools.reduce(jnp.maximum, highs)
    center = (emax + emin) * 0.5
    half = 0.55 * (emax - emin)
    offset = (shift - center) / half
    factor = scale / half

    def apply(coefs):
        out = []
        for l in range(len(coefs) + 1):
            value = zero
            if l < len(coefs):
                value = value + offset * coefs[l]
            if l + 1 < len(coefs):
                value = value + factor * coefs[l + 1]
            if l:
                value = value + factor * coefs[l - 1]
            out.append(value)
        return out

    terms = [[zero + 1.0]]
    terms.append(apply(terms[0]))
    for m in range(2, 7):
        nxt = apply(terms[-1])
        old = terms[-2]
        terms.append(
            [2.0 * v - (old[l] if l < len(old) else zero) for l, v in enumerate(nxt)]
        )
    diag, offd, out = zero, zero, zero
    for k in range(LANCZOS):
        diag = jnp.where(lane == k, jnp.broadcast_to(alphas[k][:, :1], lane.shape), diag)
        if k < LANCZOS - 1:
            offd = jnp.where(lane == k, jnp.broadcast_to(betas[k][:, :1], lane.shape), offd)
    for m in range(1, 7):
        value = functools.reduce(
            jnp.add, [c * normal[l] for l, c in enumerate(terms[m])]
        )
        out = jnp.where(lane == m - 1, jnp.broadcast_to(value[:, :1], lane.shape), out)
    diag_ref[...] = diag[:, :8]
    offd_ref[...] = offd[:, :7]
    moments_ref[...] = out[:, :6]

    _, core, side = sides()
    wide = [
        jnp.concatenate([jnp.broadcast_to(terms[3][l][:, :1], lane.shape)] * 2, axis=1)
        for l in range(4)
    ]
    mine = [jnp.where(core == 1, w[1:2], w[0:1]) for w in wide]
    other = [jnp.where(core == 1, w[0:1], w[1:2]) for w in wide]

    def combine(chunk, carry):
        at = pl.ds(chunk * ROWS, ROWS)
        p2 = jnp.where(side == 0, p2_across[0, at], p2_inside[0, at])
        p0 = jnp.where(side == 0, p0_across[0, at], p0_inside[0, at])
        value = mine[0] * p0 + mine[1] * p1[side, at]
        field_ref[core, 0, at] = value + mine[2] * p2 + mine[3] * p3[side, at]
        value = other[0] * swapped[0, at]
        for l in range(1, 4):
            value = value + other[l] * swapped[l, at]
        field_ref[1 - core, 0, at] = value
        return carry

    chunks(combine, 0)


def gathered(copies, axes):
    count = copies.shape[0]
    return lax.all_to_all(copies[:, None], axes, 0, 0, tiled=True).reshape(count, 128)


def exchange(block, route):
    return lax.ppermute(block, SLAB, route)


def shards(start_vectors, levels, energies):
    devices = 512
    inside = [(i, i ^ 2) for i in range(devices)]
    across = [(i, (((i + 2) ^ 2) - 2) % devices) for i in range(devices)]
    partner = [(i, i ^ 1) for i in range(devices)]

    def pair(left, right):
        return exchange(left, across), exchange(right, inside)

    here, send, base = call(
        onsite_kernel, (PLANES, PLANES, shape(8, 256)), [VMEM] * 3, "onsite"
    )(energies.reshape(1, -1), levels, start_vectors)
    left, right, sites = call(assemble_kernel, (PLANES,) * 3, [VMEM] * 3, "assemble")(
        base, here, exchange(send, partner)
    )
    parts, ones, twos = [], [], [(left, right)]
    swapped = None
    for step in range(3):
        got = pair(left, right)
        if step:
            parts.append(summed)
        if step == 2:
            swapped = exchange(
                call(swap_kernel, shape(4, 256, 256), [VMEM] * 6, "swap")(
                    *twos[0], ones[0], *twos[1], ones[1]
                ),
                partner,
            )
        one, new_left, new_right = call(
            functools.partial(round_kernel, False), (PLANES,) * 3, [VMEM] * 6, "round"
        )(base, left, right, *got, sites)
        summed = call(
            functools.partial(sums_kernel, step == 0),
            shape(5 if step == 0 else 4, 8, 128), [VMEM] * 5, "sums",
        )(left, right, one, new_left, new_right)
        ones.append(one)
        left, right = new_left, new_right
        twos.append((left, right))
    parts.append(summed)
    got = pair(left, right)
    rows = call(
        functools.partial(round_kernel, True),
        shape(32, 128), [VMEM] * 9, "round_last", [pltpu.VMEM((2, 256, 256), jnp.float32)],
    )(base, left, right, *got, sites, *parts)
    rows = gathered(rows, STAGES[0])
    rows = call(total_kernel, shape(16, 128), [VMEM], "total")(rows)
    rows = gathered(rows, STAGES[1])
    field, diag, offd, moments, good = call(
        finish_kernel,
        (
            shape(2, 1, 256, 256), shape(2, 8), shape(2, 7), shape(2, 6),
            jax.ShapeDtypeStruct((1, 128), jnp.int32),
        ),
        [VMEM] * 9, "finish",
    )(base, rows, *twos[0], ones[0], *twos[1], ones[1], swapped)

    def accept(field, diag, offd, moments, *_):
        return (field, diag, offd, moments)

    def redo(field, diag, offd, moments, *inputs):
        return stepwise(*inputs)

    return lax.cond(
        good[0, 0] == 1, accept, redo,
        field, diag, offd, moments, start_vectors, levels, energies,
    )


def solution(mesh):
    split = Mesh(mesh.devices.reshape(8, 4, 8, 2), SLAB)
    in_specs = (P(None, SLAB, None, None), P(SLAB, None, None), P())
    out_specs = (P(None, SLAB, None, None), P(), P(), P())
    return jax.shard_map(
        shards, mesh=split, in_specs=in_specs, out_specs=out_specs, check_vma=False
    )
```

```python
import functools

import jax
import jax.numpy as jnp
from jax import lax
from jax.experimental import pallas as pl
from jax.experimental.pallas import tpu as pltpu
from jax.sharding import Mesh
from jax.sharding import PartitionSpec as P

LANCZOS = 8
SLAB = ("slab_0", "slab_1", "slab_2", "slab_3")
STAGES = (("slab_1", "slab_2"), ("slab_0", "slab_3"))
ROWS = 128
NUDGE = 1e-3
ROUNDING = 2e-7
TOLERANCE = 1e-4
VMEM = pl.BlockSpec(memory_space=pltpu.VMEM)
PARAMS = pltpu.CompilerParams(vmem_limit_bytes=24 * 1024 * 1024)


def from_behind(block, axis, distance):
    devices = range(lax.axis_size(axis))
    route = [((i - distance) % len(devices), i) for i in devices]
    return lax.ppermute(block, axis, route)


def one_axis_at_a_time(value, axes):
    for axis in axes:
        value = lax.psum(value, axis)
    return value


def inner(first, second):
    return jnp.sum(first * second, axis=(1, 2, 3))


def expand(values):
    return values[:, None, None, None]


def hamiltonian(field, onsite):
    below = from_behind(field, SLAB, 1)
    above = from_behind(field, SLAB, -1)
    beside = jnp.roll(field, 1, 2) + jnp.roll(field, -1, 2)
    beside = beside + jnp.roll(field, 1, 3) + jnp.roll(field, -1, 3)
    return onsite[None] * field - (beside + below + above)


def stepwise(start_vectors, levels, energies):
    level_ids = lax.broadcasted_iota(jnp.int32, (energies.shape[0], 1, 1, 1), 0)
    onsite = jnp.sum(
        jnp.where(levels[None] == level_ids, energies[:, None, None, None], 0.0), axis=0
    )
    vec_count = start_vectors.shape[0]
    norm0 = one_axis_at_a_time(inner(start_vectors, start_vectors), SLAB)

    def lanczos(state, step):
        vector, previous, beta_prev = state
        work = hamiltonian(vector, onsite) - expand(beta_prev) * previous
        alpha = one_axis_at_a_time(inner(vector, work), SLAB)
        work = work - expand(alpha) * vector
        beta = jnp.sqrt(one_axis_at_a_time(inner(work, work), SLAB))
        return (work / expand(beta), vector, beta), (alpha, beta)

    vector = start_vectors / expand(jnp.sqrt(norm0))
    _, (alphas, betas) = lax.scan(
        lanczos,
        (vector, jnp.zeros_like(vector), jnp.zeros((vec_count,), jnp.float32)),
        None,
        length=LANCZOS,
    )
    diag = alphas.T
    offd = betas[: LANCZOS - 1].T
    zero_col = jnp.zeros((vec_count, 1), jnp.float32)
    left = jnp.concatenate([zero_col, offd], axis=1)
    right = jnp.concatenate([offd, zero_col], axis=1)
    emin = jnp.min(diag - left - right, axis=1)
    emax = jnp.max(diag + left + right, axis=1)
    center = expand((emax + emin) * 0.5)
    half = expand(0.55 * (emax - emin))

    def scaled(field):
        return (hamiltonian(field, onsite) - center * field) / half

    term1 = scaled(start_vectors)
    term2 = 2.0 * scaled(term1) - start_vectors
    term3 = 2.0 * scaled(term2) - term1
    local = jnp.stack(
        [
            inner(start_vectors, term1),
            inner(start_vectors, term2),
            inner(start_vectors, term3),
            inner(term2, term2),
            inner(term3, term2),
            inner(term3, term3),
        ],
        axis=0,
    )
    sums = one_axis_at_a_time(local, SLAB)
    moments = (
        jnp.stack(
            [
                sums[0],
                sums[1],
                sums[2],
                2.0 * sums[3] - norm0,
                2.0 * sums[4] - sums[0],
                2.0 * sums[5] - norm0,
            ],
            axis=1,
        )
        / norm0[:, None]
    )
    return (term3, diag, offd, moments)


def shape(*dims):
    return jax.ShapeDtypeStruct(dims, jnp.float32)


PLANES = shape(2, 256, 256)
CHUNKS = 256 // ROWS
PAIR_COST = pl.CostEstimate(flops=4_000_000, bytes_accessed=4_000_000, transcendentals=0)


def call(kernel, out_shape, in_specs, scratch=()):
    return pl.pallas_call(
        kernel,
        out_shape=out_shape,
        in_specs=in_specs,
        out_specs=jax.tree.map(lambda leaf: VMEM, out_shape),
        scratch_shapes=scratch,
        compiler_params=PARAMS,
        cost_estimate=PAIR_COST,
    )


def sides():
    parity = lax.axis_index(SLAB[2]) % 2
    core = lax.axis_index(SLAB[3])
    return parity, core, jnp.where(core == parity, 0, 1)


def onsite_kernel(energies_ref, levels_ref, start, out_ref, send_ref, base_ref):
    count = energies_ref.shape[1]
    values = [
        jnp.broadcast_to(energies_ref[0:1, index : index + 1], (1, 256))
        for index in range(count)
    ]
    mean = functools.reduce(jnp.add, values) * (1.0 / count)
    spread = functools.reduce(jnp.add, [jnp.square(v - mean) for v in values])
    scale = 1.05 * jnp.sqrt(6.0 + spread * (1.0 / count))
    inverse = 1.0 / scale
    base_ref[0:1] = mean
    base_ref[1:2] = inverse
    base_ref[2:3] = scale
    values = [(v - mean) * inverse for v in values]
    core = lax.axis_index(SLAB[3])

    def rows_of(chunk, carry):
        rows = pl.ds(chunk * ROWS, ROWS)
        level = levels_ref[0, rows]
        value = jnp.zeros(level.shape, jnp.float32)
        for index in range(count):
            value = jnp.where(level == index, values[index], value)
        out_ref[0, rows] = value
        out_ref[1, rows] = start[core, 0, rows]
        send_ref[1, rows] = value
        send_ref[0, rows] = start[1 - core, 0, rows]
        return carry

    lax.fori_loop(0, CHUNKS, rows_of, 0)


def in_plane(plane, chunk):
    rows = pl.ds(chunk * ROWS, ROWS)
    before = pl.ds(pl.multiple_of((chunk * ROWS + 248) % 256, 8), 8)
    after = pl.ds(pl.multiple_of((chunk * ROWS + ROWS) % 256, 8), 8)
    middle = plane[rows]
    tall = jnp.concatenate([plane[before], middle, plane[after]], axis=0)
    beside = pltpu.roll(tall, 1, 0)[8 : 8 + ROWS]
    beside = beside + pltpu.roll(tall, ROWS + 15, 0)[8 : 8 + ROWS]
    return beside + (pltpu.roll(middle, 1, 1) + pltpu.roll(middle, 255, 1)), middle


def folded(values):
    total = values[:, :128] + values[:, 128:]
    return jnp.sum(total.reshape(ROWS // 8, 8, 128), axis=0)


def chunks(body, count):
    zero = jnp.zeros((8, 128), jnp.float32)
    return lax.fori_loop(0, CHUNKS, body, (zero,) * count)


def partial(fields, sites, prior, inverse):
    def body(chunk, carry):
        rows = pl.ds(chunk * ROWS, ROWS)
        for s in range(2):
            beside, middle = in_plane(fields[s].at[0], chunk)
            value = sites[s, rows] * middle - inverse * (beside + fields[1 - s][0, rows])
            if prior is not None:
                value = value - prior[s, rows]
            fields[s][1, rows] = value
        return carry

    chunks(body, 0)


def assemble_kernel(base_ref, here_ref, received, across_ref, inside_ref, sites_ref):
    mine = sides()[2]

    def body(chunk, carry):
        rows = pl.ds(chunk * ROWS, ROWS)
        kept, taken = here_ref[1, rows], received[0, rows]
        across_ref[0, rows] = jnp.where(mine == 0, kept, taken)
        inside_ref[0, rows] = jnp.where(mine == 0, taken, kept)
        sites_ref[mine, rows] = here_ref[0, rows]
        sites_ref[1 - mine, rows] = received[1, rows]
        return carry

    chunks(body, 0)
    partial((across_ref, inside_ref), sites_ref, None, base_ref[1:2])


def half_rows(sent):
    parity = lax.axis_index(SLAB[2]) % 2
    return (parity if sent else 1 - parity) * 128


def round_kernel(kind, base_ref, across, inside, from_across, from_inside, sites, *refs):
    last = kind == "last"
    short = ()
    if last:
        parts, row_ref, one = refs[:3], refs[3], refs[4]
    else:
        one, new_across, new_inside = refs[:3]
        fields = (new_across, new_inside)
        short = refs[3:]
    own, got = (across, inside), (from_across, from_inside)
    inverse = base_ref[1:2]

    def first(chunk, carry):
        rows = pl.ds(chunk * ROWS, ROWS)
        for s in range(2):
            near = got[s][rows] if last else got[s][0, rows]
            value = own[s][1, rows] - inverse * near
            one[s, rows] = value
            if last:
                carry = (
                    carry[0] + folded(value * own[s][0, rows]),
                    carry[1] + folded(value * value),
                )
        return carry

    totals = chunks(first, 2 if last else 0)

    def second(chunk, carry):
        rows = pl.ds(chunk * ROWS, ROWS)
        for s in range(2):
            beside, middle = in_plane(one.at[s], chunk)
            field = own[s][0, rows]
            beside = beside + one[1 - s, rows]
            if not last:
                beside = beside + (got[s][1, rows] - inverse * field)
            value = sites[s, rows] * middle - inverse * beside - field
            if last:
                carry = (carry[0] + folded(value * middle),)
            else:
                fields[s][0, rows] = value
        return carry

    final = chunks(second, 1 if last else 0)
    if last:
        start = half_rows(False)

        def bonds(chunk, carry):
            rows = pl.ds(pl.multiple_of(start + chunk * ROWS, 8), ROWS)
            for s in range(2):
                edge = got[s][pl.ds(256 + chunk * ROWS, ROWS)] - inverse * own[s][0, rows]
                carry = carry - folded((2.0 * inverse) * (edge * one[s, rows]))
            return carry

        final = lax.fori_loop(0, 128 // ROWS, bonds, final[0])
        pack(parts, tuple(totals) + (final,), row_ref)
        return
    partial(fields, sites, one, inverse)
    if short:
        start = half_rows(True)

        def trim(chunk, carry):
            rows = pl.ds(chunk * ROWS, ROWS)
            for s in range(2):
                short[s][rows] = fields[s][0, rows]
            return carry

        def trim_half(chunk, carry):
            rows = pl.ds(pl.multiple_of(start + chunk * ROWS, 8), ROWS)
            for s in range(2):
                short[s][pl.ds(256 + chunk * ROWS, ROWS)] = fields[s][1, rows]
            return carry

        lax.fori_loop(0, 256 // ROWS, trim, 0)
        lax.fori_loop(0, 128 // ROWS, trim_half, 0)


def sums_kernel(first, across, inside, one, new_across, new_inside, sums):
    old, new = (across, inside), (new_across, new_inside)

    def body(chunk, carry):
        rows = pl.ds(chunk * ROWS, ROWS)
        for s in range(2):
            field, value, later = old[s][0, rows], one[s, rows], new[s][0, rows]
            terms = [value * field, value * value, later * value, later * later]
            if first:
                terms.append(field * field)
            carry = tuple(c + folded(t) for c, t in zip(carry, terms))
        return carry

    for index, total in enumerate(chunks(body, 5 if first else 4)):
        sums[index] = total


def pack(parts, totals, row_ref):
    entries = [(0, parts[0][4])]
    for index in range(3):
        places = (8 + 2 * index, 2 * index + 1, 9 + 2 * index, 2 * index + 2)
        entries += [(place, parts[index][k]) for k, place in enumerate(places)]
    entries += list(zip((14, 7, 15), totals))
    lane = lax.broadcasted_iota(jnp.int32, (1, 128), 1)
    row = jnp.zeros((1, 128), jnp.float32)
    for place, value in entries:
        total = jnp.sum(jnp.sum(value, axis=0, keepdims=True), axis=1, keepdims=True)
        row = jnp.where(lane == place, total, row)
    row_ref[...] = jnp.broadcast_to(row, row_ref.shape)


def total_kernel(rows_ref, out_ref):
    total = jnp.sum(rows_ref[...], axis=0, keepdims=True)
    out_ref[...] = jnp.broadcast_to(total, out_ref.shape)


def swap_kernel(p0_across, p0_inside, p1, p2_across, p2_inside, p3, out_ref):
    other = 1 - sides()[2]

    def body(chunk, carry):
        rows = pl.ds(chunk * ROWS, ROWS)
        out_ref[0, rows] = jnp.where(other == 0, p0_across[0, rows], p0_inside[0, rows])
        out_ref[1, rows] = p1[other, rows]
        out_ref[2, rows] = jnp.where(other == 0, p2_across[0, rows], p2_inside[0, rows])
        out_ref[3, rows] = p3[other, rows]
        return carry

    chunks(body, 0)


def finish_kernel(
    base_ref, rows_ref, p0_across, p0_inside, p1, p2_across, p2_inside, p3, swapped,
    field_ref, diag_ref, offd_ref, moments_ref, good_ref,
):
    shift, scale = base_ref[0:1, :128], base_ref[2:3, :128]
    lane = lax.broadcasted_iota(jnp.int32, (2, 128), 1)
    rows = rows_ref[...]
    sub = lax.broadcasted_iota(jnp.int32, rows.shape, 0)
    even = jnp.sum(jnp.where(sub % 2 == 0, rows, 0.0), axis=0, keepdims=True)
    odd = jnp.sum(jnp.where(sub % 2 == 1, rows, 0.0), axis=0, keepdims=True)
    total = jnp.concatenate([even, odd], axis=0)

    def column(index):
        return jnp.broadcast_to(total[:, index : index + 1], (2, 128))

    plain = [column(index) for index in range(8)]
    largest = [jnp.maximum(plain[k], plain[min(k + 1, 7)]) for k in range(8)]
    square = [
        plain[k] + jnp.where(lane == k + 1, NUDGE * plain[k], 0.0) for k in range(8)
    ]
    cross = [
        column(8 + k) + jnp.where(lane == k + 9, NUDGE * largest[k], 0.0) for k in range(8)
    ]
    moment = []
    for k in range(8):
        moment.append(square[k] - square[k - 1] if k else square[k])
        moment.append(cross[k] - cross[k - 1] if k else cross[k])
    norm0 = moment[0]
    sigma = [value / norm0 for value in moment]
    normal = list(sigma)
    zero = jnp.zeros_like(norm0)
    older = [zero] * len(sigma)
    alphas, betas = [], []
    weight = zero
    for k in range(LANCZOS):
        size = len(sigma)
        pushed = [
            (sigma[l + 1] + sigma[l - 1]) if l else sigma[1] for l in range(size - 1)
        ]
        ratio = (pushed[k] - weight * older[k]) / sigma[k]
        alphas.append(ratio)
        if k < LANCZOS - 1:
            fresh = [
                pushed[l] - ratio * sigma[l] - weight * older[l] for l in range(size - 1)
            ]
            weight = fresh[k + 1] / sigma[k]
            betas.append(jnp.sqrt(weight))
            older, sigma = sigma, fresh
    alphas = [scale * value + shift for value in alphas]
    betas = [scale * value for value in betas]

    def spread(values):
        error, norm = zero, zero
        for value in values:
            exact = jnp.broadcast_to(value[:, :1], value.shape)
            error = error + jnp.square(
                jnp.broadcast_to(
                    jnp.sum(jnp.abs(value - exact), axis=1, keepdims=True), value.shape
                )
            )
            norm = norm + jnp.square(exact)
        error = jnp.sum(error, axis=0, keepdims=True)
        norm = jnp.sum(norm, axis=0, keepdims=True)
        allowed = TOLERANCE * NUDGE / ROUNDING
        return jnp.where(error <= allowed * allowed * norm, 1, 0)

    fits = jnp.minimum(spread(alphas), spread(betas))
    good_ref[...] = jnp.broadcast_to(fits[0:1], good_ref.shape)

    lows, highs = [], []
    for k in range(LANCZOS):
        left = betas[k - 1] if k else zero
        right = betas[k] if k < LANCZOS - 1 else zero
        lows.append(alphas[k] - left - right)
        highs.append(alphas[k] + left + right)
    emin = functools.reduce(jnp.minimum, lows)
    emax = functools.reduce(jnp.maximum, highs)
    center = (emax + emin) * 0.5
    half = 0.55 * (emax - emin)
    offset = (shift - center) / half
    factor = scale / half

    def apply(coefs):
        out = []
        for l in range(len(coefs) + 1):
            value = zero
            if l < len(coefs):
                value = value + offset * coefs[l]
            if l + 1 < len(coefs):
                value = value + factor * coefs[l + 1]
            if l:
                value = value + factor * coefs[l - 1]
            out.append(value)
        return out

    terms = [[zero + 1.0]]
    terms.append(apply(terms[0]))
    for _ in range(2, 7):
        nxt = apply(terms[-1])
        old = terms[-2]
        terms.append(
            [2.0 * v - (old[l] if l < len(old) else zero) for l, v in enumerate(nxt)]
        )
    diag, offd, out = zero, zero, zero
    for k in range(LANCZOS):
        diag = jnp.where(lane == k, jnp.broadcast_to(alphas[k][:, :1], lane.shape), diag)
        if k < LANCZOS - 1:
            offd = jnp.where(lane == k, jnp.broadcast_to(betas[k][:, :1], lane.shape), offd)
    for m in range(1, 7):
        value = functools.reduce(
            jnp.add, [c * normal[l] for l, c in enumerate(terms[m])]
        )
        out = jnp.where(lane == m - 1, jnp.broadcast_to(value[:, :1], lane.shape), out)
    diag_ref[...] = diag[:, :8]
    offd_ref[...] = offd[:, :7]
    moments_ref[...] = out[:, :6]

    _, core, side = sides()
    wide = [
        jnp.concatenate([jnp.broadcast_to(terms[3][l][:, :1], lane.shape)] * 2, axis=1)
        for l in range(4)
    ]
    mine = [jnp.where(core == 1, w[1:2], w[0:1]) for w in wide]
    other = [jnp.where(core == 1, w[0:1], w[1:2]) for w in wide]

    def combine(chunk, carry):
        at = pl.ds(chunk * ROWS, ROWS)
        p2 = jnp.where(side == 0, p2_across[0, at], p2_inside[0, at])
        p0 = jnp.where(side == 0, p0_across[0, at], p0_inside[0, at])
        value = mine[0] * p0 + mine[1] * p1[side, at]
        field_ref[core, 0, at] = value + mine[2] * p2 + mine[3] * p3[side, at]
        value = other[0] * swapped[0, at]
        for l in range(1, 4):
            value = value + other[l] * swapped[l, at]
        field_ref[1 - core, 0, at] = value
        return carry

    chunks(combine, 0)


def gathered(copies, axes):
    count = copies.shape[0]
    return lax.all_to_all(copies[:, None], axes, 0, 0, tiled=True).reshape(count, 128)


def exchange(block, route):
    return lax.ppermute(block, SLAB, route)


def shards(start_vectors, levels, energies):
    devices = 512
    inside = [(i, i ^ 2) for i in range(devices)]
    across = [(i, (((i + 2) ^ 2) - 2) % devices) for i in range(devices)]
    partner = [(i, i ^ 1) for i in range(devices)]

    def pair(left, right):
        far = exchange(left, across)
        return far, exchange(right, inside)

    here, send, base = call(
        onsite_kernel, (PLANES, PLANES, shape(8, 256)), [VMEM] * 3
    )(energies.reshape(1, -1), levels, start_vectors)
    left, right, sites = call(assemble_kernel, (PLANES,) * 3, [VMEM] * 3)(
        base, here, exchange(send, partner)
    )
    parts, ones, twos = [], [], [(left, right)]
    swapped = None
    for step in range(3):
        got = pair(left, right)
        if step:
            parts.append(summed)
        if step == 2:
            swapped = exchange(
                call(swap_kernel, shape(4, 256, 256), [VMEM] * 6)(
                    *twos[0], ones[0], *twos[1], ones[1]
                ),
                partner,
            )
        one, new_left, new_right, *short = call(
            functools.partial(round_kernel, "round"),
            (PLANES,) * 3 + (shape(384, 256),) * (2 if step == 2 else 0),
            [VMEM] * 6,
        )(base, left, right, *got, sites)
        summed = call(
            functools.partial(sums_kernel, step == 0),
            shape(5 if step == 0 else 4, 8, 128), [VMEM] * 5,
        )(left, right, one, new_left, new_right)
        ones.append(one)
        left, right = new_left, new_right
        twos.append((left, right))
    parts.append(summed)
    got = pair(*short)
    rows = call(
        functools.partial(round_kernel, "last"),
        shape(32, 128), [VMEM] * 9, [pltpu.VMEM((2, 256, 256), jnp.float32)],
    )(base, left, right, *got, sites, *parts)
    rows = gathered(rows, STAGES[0])
    rows = call(total_kernel, shape(16, 128), [VMEM])(rows)
    rows = gathered(rows, STAGES[1])
    field, diag, offd, moments, good = call(
        finish_kernel,
        (
            shape(2, 1, 256, 256), shape(2, 8), shape(2, 7), shape(2, 6),
            jax.ShapeDtypeStruct((1, 128), jnp.int32),
        ),
        [VMEM] * 9,
    )(base, rows, *twos[0], ones[0], *twos[1], ones[1], swapped)

    def accept(field, diag, offd, moments, *_):
        return (field, diag, offd, moments)

    def redo(field, diag, offd, moments, *inputs):
        return stepwise(*inputs)

    return lax.cond(
        good[0, 0] == 1, accept, redo,
        field, diag, offd, moments, start_vectors, levels, energies,
    )


def solution(mesh):
    split = Mesh(mesh.devices.reshape(8, 4, 8, 2), SLAB)
    in_specs = (P(None, SLAB, None, None), P(SLAB, None, None), P())
    out_specs = (P(None, SLAB, None, None), P(), P(), P())

    return jax.shard_map(
        shards, mesh=split, in_specs=in_specs, out_specs=out_specs, check_vma=False
    )
```
